128 devices in a mesh: ty: 8 (over x, core), tx: 16 (over z, y).
Axes of the slice: x: 4, y: 4, z: 4, core: 2. Of those that a mesh axis runs over, the one named last changes fastest.
Arguments:
- velocity: float32 [2, 3, 1024, 2048], P(None, None, 'ty', 'tx'), may hold values from -6 to 6
- start_position: float32 [2, 65536], P(None, ('ty', 'tx')), may hold values from 0 to 128, as said below
- cells: int32 [2, 4, 2, 65536], P(None, None, None, ('ty', 'tx')), may hold values from -1 to 127, as said below
- history: float32 [2, 71, 65536], P(None, None, ('ty', 'tx')), may hold values from -6 to 6
- leavers: int32 [1, 8], replicated, may hold values from 1 to 16, as said below
- owner: int32 [65536, 1], P(('ty', 'tx')), may hold values from 0 to 127; in each aligned block of 512 rows (0 to 511, 512 to 1023, ...) at most 16 rows name the same one
- filter_matrix: float32 [73, 73], replicated, may hold values from -0.75 to 0.75
Outputs:
- filtered: float32 [2, 73, 262144], P(None, None, ('ty', 'tx'))
The draws below stay inside these ranges and needn't reach their ends.
Inputs may be any that keep to these rules, and one draw needn't show every extreme that they name: `start_position`: coordinates in cell units of the particle's tile. First coordinate cells lie in -1 .. 127 and second in -1 .. 127. Each move has one direction with exactly 16 leavers. Among the 512 slots of one tile no owner appears more than 16 times.
All inputs are finite; a program needn't handle non-finite values.
Results may differ from the reference program's by a relative error of at most 0.0003.
Values sent between devices are 32-bit elements; how exact they have to be, the bound alone decides.
A program may use at most 64 MiB of HBM per device.

```python
import math
import jax
import jax.numpy as jnp
import numpy as np
from jax import lax

CY = 128
CX = 128
P_SIZE = 512
STEPS = 2
SAMPLES = 73
HISTORY = 71
MOST = 16
TILES = 128
SEND = 16
NY = 1024
NX = 2048
N_TY = 8
N_TX = 16


moves = ((-1, -1), (-1, 0), (-1, 1), (0, -1), (0, 1), (1, -1), (1, 0), (1, 1))


def plan_draw(key):
    base_key = jax.random.fold_in(key, 9117)
    key_count, key_pick, key_rows, key_cols, key_walk = jax.random.split(base_key, 5)
    counts = jax.random.randint(key_count, (STEPS - 1, 8), 1, MOST + 1)
    pick = jax.random.randint(key_pick, (STEPS - 1, 1), 0, 8)
    counts = jnp.where(jnp.arange(8)[None, :] == pick, MOST, counts).astype(jnp.int32)
    slot = jnp.arange(P_SIZE, dtype=jnp.int32)
    lanes = []
    for step in range(STEPS - 1):
        offsets = jnp.cumsum(counts[step]) - counts[step]
        relative = slot - step * 8 * MOST
        lanes.append([(relative >= offsets[j]) & (relative < offsets[j] + counts[step, j]) for j in range(8)])
    base_y = jax.random.randint(key_rows, (TILES, P_SIZE), 0, CY)
    base_x = jax.random.randint(key_cols, (TILES, P_SIZE), 0, CX)
    for step in range(STEPS - 1):
        for j in range(8):
            dy, dx = moves[j]
            if dy == 1:
                base_y = jnp.where(lanes[step][j], CY - 1, base_y)
            if dy == -1:
                base_y = jnp.where(lanes[step][j], 0, base_y)
            if dx == 1:
                base_x = jnp.where(lanes[step][j], CX - 1, base_x)
            if dx == -1:
                base_x = jnp.where(lanes[step][j], 0, base_x)
    current_y = base_y
    current_x = base_x
    cell_list = []
    for step in range(STEPS):
        section_list = []
        for section in range(4):
            rolls = jax.random.randint(jax.random.fold_in(key_walk, step * 4 + section), (2, TILES, P_SIZE), 0, 5)
            delta = (rolls == 4).astype(jnp.int32) - (rolls == 0).astype(jnp.int32)
            cell_y = jnp.clip(current_y + delta[0], -1, CY - 1)
            cell_x = jnp.clip(current_x + delta[1], -1, CX - 1)
            section_list.append(jnp.stack([cell_y.reshape(-1), cell_x.reshape(-1)]))
        cell_list.append(jnp.stack(section_list))
        if step < STEPS - 1:
            grid_y = current_y.reshape(N_TY, N_TX, P_SIZE)
            grid_x = current_x.reshape(N_TY, N_TX, P_SIZE)
            new_y = grid_y
            new_x = grid_x
            for j in range(8):
                dy, dx = moves[j]
                rolled_y = jnp.clip(jnp.roll(grid_y, (dy, dx), axis=(0, 1)) - dy * CY, -1, CY - 1)
                rolled_x = jnp.clip(jnp.roll(grid_x, (dy, dx), axis=(0, 1)) - dx * CX, -1, CX - 1)
                new_y = jnp.where(lanes[step][j], rolled_y, new_y)
                new_x = jnp.where(lanes[step][j], rolled_x, new_x)
            current_y = new_y.reshape(TILES, P_SIZE)
            current_x = new_x.reshape(TILES, P_SIZE)
    cell_array = jnp.stack(cell_list).astype(jnp.int32)
    return (counts, base_y, base_x, cell_array)


def draw_leavers(key, part):
    counts, base_y, base_x, cell_array = plan_draw(key)
    return counts


def draw_cells(key, part):
    counts, base_y, base_x, cell_array = plan_draw(key)
    return cell_array


def draw_start_position(key, part):
    counts, base_y, base_x, cell_array = plan_draw(key)
    uniform = jax.random.uniform(jax.random.fold_in(key, 4242), (2, TILES, P_SIZE), jnp.float32)
    fraction = 0.999 * uniform
    rows = base_y.astype(jnp.float32) + fraction[0]
    cols = base_x.astype(jnp.float32) + fraction[1]
    return jnp.stack([rows.reshape(-1), cols.reshape(-1)]).astype(jnp.float32)


def steps_of(stream_key, shape, shards, low, largest):
    def one(position, shards_of):
        steps = jax.random.uniform(jax.random.fold_in(jax.random.fold_in(stream_key, 6), position), (shards_of,), jnp.float32, low / len(shards), largest / len(shards))
        return jnp.repeat(jnp.exp(steps), shape[position] // shards_of).reshape((-1,) + (1,) * (len(shape) - position - 1))

    loudness = one(*shards[0])
    for cut in shards[1:]:
        loudness = loudness * one(*cut)
    return loudness


def shared_out(stream_key, own, number, rows, count, top, bound, skew):
    ranking = jax.random.permutation(stream_key, count)
    crowded, ordinary = portions_of(count, rows * top, bound, skew, True), portions_of(count, rows * top, bound, skew, False)
    places = jnp.arange(count)

    def named(sizes, offset_by):
        used = int((sizes > 0).sum())
        fixed = max(1, used // 4)
        moved = fixed + (places - fixed + offset_by * (used - fixed)) % max(1, count - fixed)
        return jnp.zeros((count,), jnp.int32).at[ranking[jnp.where(places < fixed, places, moved)]].set(jnp.asarray(sizes, jnp.int32))

    sizes = jnp.where(number % 4 == 0, named(crowded, number // 4), named(ordinary, number - number // 4 - 1))
    mixed = jax.random.permutation(jax.random.fold_in(own, 3), count)
    giver, taker = mixed[0:count // 2 * 2:2], mixed[1:count // 2 * 2:2]
    margin = jnp.minimum(sizes[giver] - 1, bound - sizes[taker]) // 2
    margin = jnp.where((giver == ranking[0]) | (taker == ranking[0]) | (sizes[taker] == 0), 0, jnp.maximum(margin, 0))
    moved = jax.random.randint(jax.random.fold_in(own, 4), (count // 2,), 0, 1 << 20) % (margin + 1)
    sizes = sizes.at[giver].add(-moved).at[taker].add(moved)
    members = jnp.searchsorted(jnp.cumsum(sizes), jnp.arange(rows * top), side="right").astype(jnp.int32)
    listing = members.reshape(top, rows).T
    listing = listing[jax.random.permutation(jax.random.fold_in(own, 1), rows)]
    offset_by = jax.random.randint(jax.random.fold_in(own, 2), (rows, 1), 0, top)
    return jnp.take_along_axis(listing, (jnp.arange(top)[None, :] + offset_by) % top, axis=1)


def portions_of(number_of, total, limit, slope, full):
    loads = [(1 << 20) // math.isqrt(rank ** slope) + 1 for rank in range(1, number_of + 1)]
    largest = limit if full else min(limit, max(-(-total // number_of), total * loads[0] // sum(loads)))
    least = 1 if total - largest >= number_of - 1 else 0
    given, surplus = [largest] + [least] * (number_of - 1), total - largest - least * (number_of - 1)
    while surplus > 0:
        free = [i for i in range(1, number_of) if given[i] < largest] or [i for i in range(1, number_of) if given[i] < limit]
        mass, remaining = sum([loads[i] for i in free]), surplus
        for i in free:
            addition = min(limit - given[i], max(1, remaining * loads[i] // mass), surplus)
            given[i] = given[i] + addition
            surplus = surplus - addition
    return np.array(given)


def noise(rng, extent, spread, bound, cuts=(), kind=jnp.bfloat16):
    values = jax.random.normal(rng, extent, jnp.float32) * spread
    if len(cuts) > 0:
        values = steps_of(rng, extent, cuts, -0.22, 0.18) * values
    return jnp.clip(values, min=-bound, max=bound).astype(kind)


def setup_inputs(seed: int = 0) -> dict:
    seeds = jax.random.split(jax.random.key(seed), 8)
    velocity = noise(seeds[0], (2, STEPS + 1, NY, NX), 1.0, 6.0, ((2, 8), (3, 16)), jnp.float32)
    start_position = draw_start_position(jax.random.fold_in(seeds[7], 71), 0)
    cells = draw_cells(jax.random.fold_in(seeds[7], 71), 0)
    history = noise(seeds[3], (2, HISTORY, TILES * P_SIZE), 1.0, 6.0, ((2, 128),), jnp.float32)
    leavers = draw_leavers(jax.random.fold_in(seeds[7], 71), 0)
    owner_keys = jax.random.split(jax.random.fold_in(seeds[5], 1), (TILES * P_SIZE) // P_SIZE)
    owner_turns = jax.random.permutation(jax.random.fold_in(seeds[5], 3), (TILES * P_SIZE) // P_SIZE)
    owner = jax.vmap(lambda own, number: shared_out(jax.random.fold_in(seeds[5], 2), own, number, P_SIZE, TILES, 1, SEND, 2))(owner_keys, owner_turns).reshape((TILES * P_SIZE, 1))
    filter_matrix = noise(seeds[6], (SAMPLES, SAMPLES), SAMPLES ** -0.5, 0.75, (), jnp.float32)
    return dict(velocity=velocity, start_position=start_position, cells=cells, history=history, leavers=leavers, owner=owner, filter_matrix=filter_matrix)


drift = 0.2
moves = ((-1, -1), (-1, 0), (-1, 1), (0, -1), (0, 1), (1, -1), (1, 0), (1, 1))


def bilinear(plane, point, cell, tile_y, tile_x):
    row = (tile_y * CY + cell[0]) % NY
    col = (tile_x * CX + cell[1]) % NX
    row_next = (row + 1) % NY
    col_next = (col + 1) % NX
    wy = point[0] - cell[0].astype(jnp.float32)
    wx = point[1] - cell[1].astype(jnp.float32)
    first = jnp.take(plane, row * NX + col, axis=1)
    second = jnp.take(plane, row * NX + col_next, axis=1)
    third = jnp.take(plane, row_next * NX + col, axis=1)
    fourth = jnp.take(plane, row_next * NX + col_next, axis=1)
    return (1.0 - wy) * ((1.0 - wx) * first + wx * second) + wy * ((1.0 - wx) * third + wx * fourth)


def rank_rows(owned):
    labels = jnp.arange(N_TY * N_TX, dtype=jnp.int32)[:, None]
    onehot = (owned[None, :] == labels).astype(jnp.int32)
    running = jnp.cumsum(onehot, axis=1)
    return jnp.sum(running * onehot, axis=0) - 1


def reference(velocity, start_position, cells, history, leavers, owner, filter_matrix):
    tiles = N_TY * N_TX
    tile = jnp.arange(tiles, dtype=jnp.int32)[:, None]
    tile_y = tile // N_TX
    tile_x = tile % N_TX
    planes = [velocity[:, a].reshape(2, NY * NX) for a in range(STEPS + 1)]
    point = start_position.reshape(2, tiles, P_SIZE)
    series = jnp.concatenate([history.reshape(2, HISTORY, tiles, P_SIZE), jnp.zeros((2, STEPS, tiles, P_SIZE), jnp.float32)], axis=1)
    slot = jnp.arange(P_SIZE, dtype=jnp.int32)
    for step in range(STEPS):
        section_cells = cells[step].reshape(4, 2, tiles, P_SIZE)
        k_one = bilinear(planes[step], point, section_cells[0], tile_y, tile_x)
        spot = point + (0.5 * drift) * k_one
        k_two = 0.5 * (bilinear(planes[step], spot, section_cells[1], tile_y, tile_x) + bilinear(planes[step + 1], spot, section_cells[1], tile_y, tile_x))
        spot = point + (0.5 * drift) * k_two
        k_three = 0.5 * (bilinear(planes[step], spot, section_cells[2], tile_y, tile_x) + bilinear(planes[step + 1], spot, section_cells[2], tile_y, tile_x))
        spot = point + drift * k_three
        k_four = bilinear(planes[step + 1], spot, section_cells[3], tile_y, tile_x)
        series = series.at[:, HISTORY + step].set(k_one)
        point = point + (drift / 6.0) * (k_one + 2.0 * k_two + 2.0 * k_three + k_four)
        if step < STEPS - 1:
            counts = leavers[step]
            offsets = jnp.cumsum(counts) - counts
            band = step * 8 * MOST
            grid_point = point.reshape(2, N_TY, N_TX, P_SIZE)
            grid_series = series.reshape(2, SAMPLES, N_TY, N_TX, P_SIZE)
            new_point = grid_point
            new_series = grid_series
            for j in range(8):
                dy, dx = moves[j]
                lane = (slot >= band + offsets[j]) & (slot < band + offsets[j] + counts[j])
                rolled = jnp.roll(grid_point, (dy, dx), axis=(1, 2))
                shift_vec = jnp.array([dy * CY, dx * CX], jnp.float32).reshape(2, 1, 1, 1)
                new_point = jnp.where(lane, rolled - shift_vec, new_point)
                new_series = jnp.where(lane, jnp.roll(grid_series, (dy, dx), axis=(2, 3)), new_series)
            point = new_point.reshape(2, tiles, P_SIZE)
            series = new_series.reshape(2, SAMPLES, tiles, P_SIZE)
    low = jnp.einsum("tj,cjn->ctn", filter_matrix, series.reshape(2, SAMPLES, tiles * P_SIZE), precision=lax.Precision.HIGHEST)
    owned = owner.reshape(tiles, P_SIZE)
    ranks = lax.map(rank_rows, owned)
    dest = owned * (4 * P_SIZE) + tile * SEND + ranks
    result = jnp.zeros((2, SAMPLES, tiles * 4 * P_SIZE), jnp.float32)
    return result.at[:, :, dest.reshape(-1)].set(low)
```

```python
import jax
import jax.numpy as jnp
from jax import lax
from jax.experimental import pallas as pl
from jax.experimental.pallas import tpu as pltpu
from jax.sharding import PartitionSpec as P

STEPS = 2
SAMPLES = 73
HISTORY = 71
MOST = 16
ROWS = 19

drift = 0.2
moves = ((-1, -1), (-1, 0), (-1, 1), (0, -1), (0, 1), (1, -1), (1, 0), (1, 1))
MESH = pl.DeviceIdType.MESH
f32 = jnp.float32
bf16 = jnp.bfloat16
i32 = jnp.int32
NT = (((1,), (1,)), ((), ()))
TN = (((0,), (0,)), ((), ()))


def iota(shape, dim):
    return lax.broadcasted_iota(i32, shape, dim)


def halves(x):
    high = x.astype(bf16)
    return high, (x - high.astype(f32)).astype(bf16)


def dot(a, b, dims=(((1,), (0,)), ((), ()))):
    return lax.dot_general(a, b, dims, preferred_element_type=f32)


def swap_blocks(x):
    sub = iota((8, 128), 0)
    block = iota((8, 128), 1) // 16
    for b in (1, 2, 4):
        row_bit = (sub // b) % 2
        col_bit = (block // b) % 2
        down = pltpu.roll(pltpu.roll(x, b, 0), 128 - 16 * b, 1)
        up = pltpu.roll(pltpu.roll(x, 8 - b, 0), 16 * b, 1)
        x = jnp.where(row_bit > col_bit, down, jnp.where(row_bit < col_bit, up, x))
    return x


def lookup(table, index):
    held = jnp.minimum(jnp.maximum(index, 0), 127)
    parts = []
    for n in range(4):
        at = jnp.broadcast_to(held[:, 128 * n : 128 * n + 128], (8, 128))
        parts.append(jnp.take_along_axis(table, at, axis=1))
    return jnp.concatenate(parts, axis=1)


def advance_kernel(
    leavers_ref, velocity_ref, start_ref, cells_ref, history_ref, owner_col_ref, owner_row_ref, filter_ref,
    arrived_ref, end_ref,
    planes, edges, edges_in, packed, packed_in, spots, spots_in, corners, split_low, message,
    edge_send, edge_recv, packed_send, packed_recv, spot_send, spot_recv, send_sem, recv_sem, own_sem,
):
    ty = lax.axis_index("ty")
    tx = lax.axis_index("tx")
    me = ty * 16 + tx
    barrier = pltpu.get_barrier_semaphore()

    def greet(k, carry):
        peer = lax.rem(me + k, 128)
        pl.semaphore_signal(barrier, inc=1, device_id=(peer // 16, lax.rem(peer, 16)), device_id_type=MESH)
        return carry

    lax.fori_loop(1, 128, greet, 0)

    def neighbour(j):
        dy, dx = moves[j]
        return (lax.rem(ty + dy + 8, 8), lax.rem(tx + dx + 16, 16))

    for a in range(3):
        for c in range(2):
            high, low = halves(velocity_ref[c, a])
            planes[2 * a, 128 * c : 128 * c + 128, 0:128] = high
            planes[2 * a, 128 * c : 128 * c + 128, 128:256] = low
    pick_row = iota((8, 256), 0)
    pick_lane = iota((8, 256), 1) % 128
    pick = ((pick_lane == 0) & (pick_row == 0)) | ((pick_lane == 127) & (pick_row == 1))
    pick = jnp.where(pick, 1.0, 0.0).astype(bf16)
    for a in range(3):
        sides = dot(pick, planes[2 * a], NT)
        for c in range(2):
            r = 3 * c + a
            edges[0, r : r + 1, :] = velocity_ref[c, a, 0:1, :]
            edges[1, r : r + 1, :] = velocity_ref[c, a, 127:128, :]
            edges[2, r : r + 1, :] = sides[0:1, 128 * c : 128 * c + 128]
            edges[3, r : r + 1, :] = sides[1:2, 128 * c : 128 * c + 128]
    for kind in range(4):
        edges[kind, 6:8, :] = jnp.zeros((2, 128), f32)

    counts = [leavers_ref[0, j] for j in range(8)]
    starts = [0]
    for j in range(8):
        starts.append(starts[j] + counts[j])
    place = iota((128, 128), 0) % 16
    way = iota((128, 128), 0) // 16
    first = jnp.zeros((128, 128), i32)
    many = jnp.zeros((128, 128), i32)
    for j in range(8):
        first = jnp.where(way == j, starts[j], first)
        many = jnp.where(way == j, counts[j], many)
    leaving = (iota((128, 128), 1) == first + place) & (place < many)
    leaving = jnp.where(leaving, 1.0, 0.0).astype(bf16)
    for c in range(2):
        high, low = halves(history_ref[c, :, 0:128])
        block = dot(leaving, high, NT) + dot(leaving, low, NT)
        packed[:, :, 128 * c : 128 * c + HISTORY] = block.reshape(8, 16, HISTORY)

    pl.semaphore_wait(barrier, 127)

    edge_copies = []
    packed_copies = []
    spot_copies = []
    for j in range(8):
        dy, dx = moves[j]
        kind = {1: 1, -1: 0}.get(dy, 3 if dx == 1 else 2)
        edge_copies.append(pltpu.make_async_remote_copy(
            src_ref=edges.at[kind], dst_ref=edges_in.at[j], send_sem=edge_send.at[j], recv_sem=edge_recv.at[j],
            device_id=neighbour(j), device_id_type=MESH))
        packed_copies.append(pltpu.make_async_remote_copy(
            src_ref=packed.at[j], dst_ref=packed_in.at[j], send_sem=packed_send.at[j], recv_sem=packed_recv.at[j],
            device_id=neighbour(j), device_id_type=MESH))
        spot_copies.append(pltpu.make_async_remote_copy(
            src_ref=spots, dst_ref=spots_in.at[j], send_sem=spot_send.at[j], recv_sem=spot_recv.at[j],
            device_id=neighbour(j), device_id_type=MESH))
    for copy in edge_copies:
        copy.start()
    for copy in packed_copies:
        copy.start()

    for a in range(2):
        for c in range(2):
            high, low = halves(0.5 * (velocity_ref[c, a] + velocity_ref[c, a + 1]))
            planes[2 * a + 1, 128 * c : 128 * c + 128, 0:128] = high
            planes[2 * a + 1, 128 * c : 128 * c + 128, 128:256] = low

    def gather(section, carry):
        plane = planes[2 * (section // 4) + (section % 4 + 1) // 2]
        cell_y = cells_ref[2 * section]
        cell_x = cells_ref[2 * section + 1]
        column = iota((256, 512), 0) % 128
        row = iota((128, 512), 0)
        for dx in range(2):
            chosen = jnp.where(column == cell_x + dx, 1.0, 0.0).astype(bf16)
            along = dot(plane, chosen)
            for dy in range(2):
                on = row == cell_y + dy
                for c in range(2):
                    part = jnp.where(on, along[128 * c : 128 * c + 128], 0.0)
                    at = 4 * dy + 2 * dx + c
                    corners[section, at : at + 1, :] = jnp.sum(part, axis=0, keepdims=True)
        return carry

    lax.fori_loop(0, 8, gather, 0)

    same = (owner_col_ref[...] == owner_row_ref[...]) & (iota((512, 512), 0) < iota((512, 512), 1))
    rank = jnp.sum(jnp.where(same, 1.0, 0.0), axis=0, keepdims=True).astype(i32)
    target = owner_row_ref[...] * 16 + rank

    for copy in edge_copies:
        copy.wait_recv()
    where_from = {move: j for j, move in enumerate(moves)}
    top = edges_in[where_from[(1, 0)]]
    bottom = edges_in[where_from[(-1, 0)]]
    left = edges_in[where_from[(0, 1)]]
    right = edges_in[where_from[(0, -1)]]
    top_left = edges_in[where_from[(1, 1)]][:, 127:128]
    top_right = edges_in[where_from[(1, -1)]][:, 0:1]
    bottom_left = edges_in[where_from[(-1, 1)]][:, 127:128]
    bottom_right = edges_in[where_from[(-1, -1)]][:, 0:1]

    def cell_of(section):
        return cells_ref[2 * section], cells_ref[2 * section + 1]

    def all_corners(section):
        step, part = section // 4, section % 4
        cell_y, cell_x = cell_of(section)
        sides = {}
        for dy in range(2):
            yy = cell_y + dy
            sides[dy] = (lookup(left, yy), lookup(right, yy))
        result = []
        ends = {}
        for dx in range(2):
            xx = cell_x + dx
            ends[dx] = tuple(
                jnp.where(xx < 0, lower, jnp.where(xx > 127, upper, lookup(line, xx)))
                for line, lower, upper in ((top, top_left, top_right), (bottom, bottom_left, bottom_right)))
        for dy in range(2):
            for dx in range(2):
                yy, xx = cell_y + dy, cell_x + dx
                outer = jnp.where(xx < 0, sides[dy][0], jnp.where(xx > 127, sides[dy][1], 0.0))
                outer = jnp.where(yy < 0, ends[dx][0], jnp.where(yy > 127, ends[dx][1], outer))
                rows = []
                for c in range(2):
                    a = step + (part == 3)
                    value = outer[3 * c + a : 3 * c + a + 1]
                    if part in (1, 2):
                        value = 0.5 * (value + outer[3 * c + a + 1 : 3 * c + a + 2])
                    rows.append(value)
                at = 4 * dy + 2 * dx
                result.append(corners[section, at : at + 2, :] + jnp.concatenate(rows, axis=0))
        return result

    def sample(section, held, point):
        cell_y, cell_x = cell_of(section)
        wy = point[0:1] - cell_y.astype(f32)
        wx = point[1:2] - cell_x.astype(f32)
        first_c, second_c, third_c, fourth_c = held
        return (1.0 - wy) * ((1.0 - wx) * first_c + wx * second_c) + wy * ((1.0 - wx) * third_c + wx * fourth_c)

    def rest_of_step(step, held, point, k_one):
        spot = point + 0.5 * drift * k_one
        k_two = sample(4 * step + 1, held[0], spot)
        spot = point + 0.5 * drift * k_two
        k_three = sample(4 * step + 2, held[1], spot)
        spot = point + drift * k_three
        k_four = sample(4 * step + 3, held[2], spot)
        return point + drift / 6.0 * (k_one + 2.0 * k_two + 2.0 * k_three + k_four)

    point = start_ref[...]
    k_first = sample(0, all_corners(0), point)
    point = rest_of_step(0, [all_corners(s) for s in (1, 2, 3)], point, k_first)

    spots[0:2, :] = point[:, 0:128]
    spots[2:4, :] = k_first[:, 0:128]
    spots[4:8, :] = jnp.zeros((4, 128), f32)
    for copy in spot_copies:
        copy.start()

    next_corners = all_corners(4)

    for copy in packed_copies:
        copy.wait_recv()
    lane = iota((1, 128), 1)
    matrix = filter_ref[...]
    partial = []
    for c in range(2):
        block = packed_in[:, :, 128 * c : 128 * c + HISTORY].reshape(128, HISTORY)
        high, low = halves(block)
        came = dot(high, leaving, TN) + dot(low, leaving, TN)
        own = jnp.where(lane < starts[8], came, history_ref[c, :, 0:128])
        series = jnp.concatenate([own, history_ref[c, :, 128:512]], axis=1)
        partial.append(lax.dot_general(
            matrix[:, 0:HISTORY], series, (((1,), (0,)), ((), ())),
            precision=lax.Precision.HIGHEST, preferred_element_type=f32))

    for copy in spot_copies:
        copy.wait_recv()
    moved_point = point[:, 0:128]
    moved_first = k_first[:, 0:128]
    for j in range(8):
        dy, dx = moves[j]
        here = (lane >= starts[j]) & (lane < starts[j + 1])
        arrival = spots_in[j]
        shift = jnp.where(iota((2, 128), 0) == 0, float(dy * 128), float(dx * 128))
        moved_point = jnp.where(here, arrival[0:2] - shift, moved_point)
        moved_first = jnp.where(here, arrival[2:4], moved_first)
    point = jnp.concatenate([moved_point, point[:, 128:512]], axis=1)
    k_first = jnp.concatenate([moved_first, k_first[:, 128:512]], axis=1)
    k_second = sample(4, next_corners, point)

    low = [
        partial[c] + matrix[:, 71:72] * k_first[c : c + 1] + matrix[:, 72:73] * k_second[c : c + 1]
        for c in range(2)
    ]
    sub = iota((16, 512), 0)
    tail = jnp.where(sub == 0, low[0][72:73], jnp.where(sub == 1, low[1][72:73], 0.0))
    for number, at, piece in (
        (0, 0, low[0][0:64]), (1, 64, low[1][0:64]),
        (2, 128, jnp.concatenate([low[0][64:72], low[1][64:72]], axis=0)), (3, 144, tail),
    ):
        high, rest = halves(piece)
        split_low[at : at + piece.shape[0], :] = high
        split_low[160 + at : 160 + at + piece.shape[0], :] = rest

    def deliver(k, carry):
        goal = lax.rem(ty + k, 8)
        chosen = jnp.where(iota((256, 512), 0) + goal * 256 == target, 1.0, 0.0).astype(bf16)
        columns = dot(split_low[...], chosen, NT)
        columns = columns[0:160] + columns[160:320]
        for h in range(2):
            owners = pl.ds(goal * 16 + 8 * h, 8)
            wide = columns[:, 128 * h : 128 * h + 128]
            message[owners, 0:16, :] = jnp.transpose(wide[0:128]).reshape(8, 16, 128)
            for a in range(3):
                message[owners, 16 + a, :] = swap_blocks(wide[128 + 8 * a : 136 + 8 * a])

        def send(m, inner):
            column = lax.rem(tx + m, 16)
            pltpu.make_async_remote_copy(
                src_ref=message.at[goal * 16 + column, pl.ds(0, ROWS)], dst_ref=arrived_ref.at[me, pl.ds(0, ROWS)],
                send_sem=send_sem, recv_sem=recv_sem, device_id=(goal, column), device_id_type=MESH).start()
            return inner

        lax.fori_loop(1 - jnp.minimum(k, 1), 16, send, 0)
        return carry

    lax.fori_loop(0, 8, deliver, 0)
    own_copy = pltpu.make_async_copy(message.at[me, pl.ds(0, ROWS)], arrived_ref.at[me, pl.ds(0, ROWS)], own_sem)
    own_copy.start()

    end_ref[...] = rest_of_step(1, [all_corners(s) for s in (5, 6, 7)], point, k_second)

    for copy in edge_copies + packed_copies + spot_copies:
        copy.wait_send()
    own_copy.wait()
    sent = message.at[pl.ds(0, 127), pl.ds(0, ROWS)]
    pltpu.make_async_copy(sent, sent, send_sem).wait()
    landed = arrived_ref.at[pl.ds(0, 127), pl.ds(0, ROWS)]
    pltpu.make_async_copy(landed, landed, recv_sem).wait()


def spread_kernel(arrived_ref, out_ref):
    wide = jnp.transpose(arrived_ref[:, 0:16, :].reshape(256, 128))
    out_ref[0, 0:64, :] = wide[0:64]
    out_ref[1, 0:64, :] = wide[64:128]
    for h in range(2):
        lanes = pl.ds(128 * h, 128)
        for a in range(3):
            part = swap_blocks(arrived_ref[8 * h : 8 * h + 8, 16 + a, :])
            if a < 2:
                out_ref[a, 64:72, lanes] = part
            else:
                out_ref[0, 72:73, lanes] = part[0:1]
                out_ref[1, 72:73, lanes] = part[1:2]


def per_device(velocity, start_position, cells, history, leavers, owner, filter_matrix):
    vmem = pl.BlockSpec(memory_space=pltpu.VMEM)
    arrived, end = pl.pallas_call(
        advance_kernel,
        out_shape=(jax.ShapeDtypeStruct((128, 24, 128), f32), jax.ShapeDtypeStruct((2, 512), f32)),
        in_specs=[pl.BlockSpec(memory_space=pltpu.SMEM)] + [vmem] * 7,
        out_specs=(pl.BlockSpec(memory_space=pl.ANY), vmem),
        scratch_shapes=[
            pltpu.VMEM((5, 256, 256), bf16),
            pltpu.VMEM((4, 8, 128), f32),
            pltpu.VMEM((8, 8, 128), f32),
            pltpu.VMEM((8, 16, 256), f32),
            pltpu.VMEM((8, 16, 256), f32),
            pltpu.VMEM((8, 128), f32),
            pltpu.VMEM((8, 8, 128), f32),
            pltpu.VMEM((8, 8, 512), f32),
            pltpu.VMEM((320, 512), bf16),
            pltpu.VMEM((128, 24, 128), f32),
        ]
        + [pltpu.SemaphoreType.DMA((8,))] * 6
        + [pltpu.SemaphoreType.DMA] * 3,
        compiler_params=pltpu.CompilerParams(collective_id=0, has_side_effects=True),
        name="advance",
    )(
        leavers, velocity, start_position, cells.reshape(16, 1, 512), history, owner,
        owner.reshape(1, 512), filter_matrix,
    )
    return pl.pallas_call(
        spread_kernel,
        grid=(8,),
        out_shape=jax.ShapeDtypeStruct((2, SAMPLES, 2048), f32),
        in_specs=[pl.BlockSpec((16, 24, 128), lambda i: (i, 0, 0))],
        out_specs=pl.BlockSpec((2, SAMPLES, 256), lambda i: (0, 0, i)),
        name="spread",
    )(arrived)


def solution(mesh):
    placed = (
        P(None, None, "ty", "tx"),
        P(None, ("ty", "tx")),
        P(None, None, None, ("ty", "tx")),
        P(None, None, ("ty", "tx")),
        P(),
        P(("ty", "tx"), None),
        P(),
    )
    return jax.shard_map(
        per_device,
        mesh=mesh,
        in_specs=placed,
        out_specs=P(None, None, ("ty", "tx")),
        check_vma=False,
    )
```

```python
import jax
import jax.numpy as jnp
from jax import lax
from jax.experimental import pallas as pl
from jax.experimental.pallas import tpu as pltpu
from jax.sharding import PartitionSpec as P

STEPS = 2
SAMPLES = 73
HISTORY = 71
MOST = 16
EARLY = 18

drift = 0.2
moves = ((-1, -1), (-1, 0), (-1, 1), (0, -1), (0, 1), (1, -1), (1, 0), (1, 1))
MESH = pl.DeviceIdType.MESH
f32 = jnp.float32
bf16 = jnp.bfloat16
i32 = jnp.int32
NT = (((1,), (1,)), ((), ()))
TN = (((0,), (0,)), ((), ()))


def iota(shape, dim):
    return lax.broadcasted_iota(i32, shape, dim)


def halves(x):
    high = x.astype(bf16)
    return high, (x - high.astype(f32)).astype(bf16)


def dot(a, b, dims=(((1,), (0,)), ((), ()))):
    return lax.dot_general(a, b, dims, preferred_element_type=f32)


def swap_blocks(x):
    sub = iota((8, 128), 0)
    block = iota((8, 128), 1) // 16
    for b in (1, 2, 4):
        row_bit = (sub // b) % 2
        col_bit = (block // b) % 2
        down = pltpu.roll(pltpu.roll(x, b, 0), 128 - 16 * b, 1)
        up = pltpu.roll(pltpu.roll(x, 8 - b, 0), 16 * b, 1)
        x = jnp.where(row_bit > col_bit, down, jnp.where(row_bit < col_bit, up, x))
    return x


def lookup(table, index):
    held = jnp.minimum(jnp.maximum(index, 0), 127)
    parts = []
    for n in range(4):
        at = jnp.broadcast_to(held[:, 128 * n : 128 * n + 128], (8, 128))
        parts.append(jnp.take_along_axis(table, at, axis=1))
    return jnp.concatenate(parts, axis=1)


def advance_kernel(
    leavers_ref, velocity_hbm, start_ref, cells_ref, history_hbm, owner_ref, filter_ref,
    slabs_ref, late_ref, end_ref,
    velocity_ref, history_ref, planes, edges, edges_in, packed, packed_in, spots, spots_in, corners,
    chosen, split_main, split_tail, split_late, message, arrived, late, late_in, slabs,
    edge_send, edge_recv, packed_send, packed_recv, spot_send, spot_recv, send_sem, recv_sem, late_sems, own_sems,
    input_sems, slab_sems,
):
    ty = lax.axis_index("ty")
    tx = lax.axis_index("tx")
    me = ty * 16 + tx
    down = [lax.rem(ty + k, 8) for k in range(8)]
    along_x = [lax.rem(tx + k, 16) for k in range(16)]
    barrier = pltpu.get_barrier_semaphore()
    load_velocity = pltpu.make_async_copy(velocity_hbm, velocity_ref, input_sems.at[0])
    load_history = pltpu.make_async_copy(history_hbm, history_ref, input_sems.at[1])
    load_velocity.start()
    load_history.start()

    def greet(k, carry):
        row = lax.rem(ty + k, 8)
        for m in range(1, 16):
            pl.semaphore_signal(barrier, inc=1, device_id=(row, along_x[m]), device_id_type=MESH)
        return carry

    lax.fori_loop(0, 8, greet, 0)
    for k in range(1, 8):
        pl.semaphore_signal(barrier, inc=1, device_id=(down[k], tx), device_id_type=MESH)

    def cell_of(section):
        both = cells_ref[section]
        return both[0:1], both[1:2]

    def neighbour(j):
        dy, dx = moves[j]
        return (down[dy % 8], along_x[dx % 16])

    def history_of(c, n):
        return history_ref[pl.ds(2 * n + c, HISTORY, stride=8), :]

    counts = [leavers_ref[0, j] for j in range(8)]
    starts = [0]
    for j in range(8):
        starts.append(starts[j] + counts[j])
    place = iota((128, 128), 0) % 16
    way = iota((128, 128), 0) // 16
    first = jnp.zeros((128, 128), i32)
    many = jnp.zeros((128, 128), i32)
    for j in range(8):
        first = jnp.where(way == j, starts[j], first)
        many = jnp.where(way == j, counts[j], many)
    leaving = (iota((128, 128), 1) == first + place) & (place < many)
    leaving = jnp.where(leaving, 1.0, 0.0).astype(bf16)

    load_velocity.wait()
    for a in range(3):
        for c in range(2):
            high, low = halves(velocity_ref[c, a])
            planes[2 * a, 128 * c : 128 * c + 128, 0:128] = high
            planes[2 * a, 128 * c : 128 * c + 128, 128:256] = low
    pick_row = iota((8, 256), 0)
    pick_lane = iota((8, 256), 1) % 128
    pick = ((pick_lane == 0) & (pick_row == 0)) | ((pick_lane == 127) & (pick_row == 1))
    pick = jnp.where(pick, 1.0, 0.0).astype(bf16)
    for a in range(3):
        sides = dot(pick, planes[2 * a], NT)
        for c in range(2):
            r = 3 * c + a
            edges[0, r : r + 1, :] = velocity_ref[c, a, 0:1, :]
            edges[1, r : r + 1, :] = velocity_ref[c, a, 127:128, :]
            edges[2, r : r + 1, :] = sides[0:1, 128 * c : 128 * c + 128]
            edges[3, r : r + 1, :] = sides[1:2, 128 * c : 128 * c + 128]
    for kind in range(4):
        edges[kind, 6:8, :] = jnp.zeros((2, 128), f32)

    load_history.wait()
    for c in range(2):
        high, low = halves(history_of(c, 0))
        block = dot(leaving, high, NT) + dot(leaving, low, NT)
        packed[:, :, 128 * c : 128 * c + HISTORY] = block.reshape(8, 16, HISTORY)

    for a in range(2):
        for c in range(2):
            high, low = halves(0.5 * (velocity_ref[c, a] + velocity_ref[c, a + 1]))
            planes[2 * a + 1, 128 * c : 128 * c + 128, 0:128] = high
            planes[2 * a + 1, 128 * c : 128 * c + 128, 128:256] = low

    def gather(section, carry):
        plane = planes[2 * (section // 4) + (section % 4 + 1) // 2]
        cell_y, cell_x = cell_of(section)
        column = iota((256, 512), 0) % 128
        row = iota((128, 512), 0)
        for dx in range(2):
            here = jnp.where(column == cell_x + dx, 1.0, 0.0).astype(bf16)
            along = dot(plane, here)
            for dy in range(2):
                on = row == cell_y + dy
                for c in range(2):
                    part = jnp.where(on, along[128 * c : 128 * c + 128], 0.0)
                    at = 4 * dy + 2 * dx + c
                    corners[section, at : at + 1, :] = jnp.sum(part, axis=0, keepdims=True)
        return carry

    lax.fori_loop(0, 8, gather, 0)

    pl.semaphore_wait(barrier, 127)

    edge_copies = []
    packed_copies = []
    spot_copies = []
    for j in range(8):
        dy, dx = moves[j]
        kind = {1: 1, -1: 0}.get(dy, 3 if dx == 1 else 2)
        edge_copies.append(pltpu.make_async_remote_copy(
            src_ref=edges.at[kind], dst_ref=edges_in.at[j], send_sem=edge_send.at[j], recv_sem=edge_recv.at[j],
            device_id=neighbour(j), device_id_type=MESH))
        packed_copies.append(pltpu.make_async_remote_copy(
            src_ref=packed.at[j], dst_ref=packed_in.at[j], send_sem=packed_send.at[j], recv_sem=packed_recv.at[j],
            device_id=neighbour(j), device_id_type=MESH))
        spot_copies.append(pltpu.make_async_remote_copy(
            src_ref=spots, dst_ref=spots_in.at[j], send_sem=spot_send.at[j], recv_sem=spot_recv.at[j],
            device_id=neighbour(j), device_id_type=MESH))
    for copy in edge_copies:
        copy.start()
    for copy in packed_copies:
        copy.start()

    named = iota((128, 512), 0) == owner_ref[...]
    before = dot(
        jnp.where(named, 1.0, 0.0).astype(bf16),
        jnp.where(iota((512, 512), 0) < iota((512, 512), 1), 1.0, 0.0).astype(bf16))
    rank = jnp.sum(jnp.where(named, before, 0.0), axis=0, keepdims=True).astype(i32)
    target = owner_ref[...] * 16 + rank

    def choose(k, carry):
        place = target - lax.rem(ty + k, 8) * 256
        chosen[k] = jnp.where(iota((256, 512), 0) == place, 1.0, 0.0).astype(bf16)
        return carry

    lax.fori_loop(0, 8, choose, 0)

    matrix = filter_ref[...]

    def keep_filtered(low, lanes):
        for c in range(2):
            high, rest = halves(low[c][0:64])
            split_main[64 * c : 64 * c + 64, lanes] = high
            split_main[128 + 64 * c : 192 + 64 * c, lanes] = rest
        high, rest = halves(jnp.concatenate([low[0][64:72], low[1][64:72]], axis=0))
        split_tail[0:16, lanes] = high
        split_tail[16:32, lanes] = rest

    def filtered(series):
        return lax.dot_general(
            matrix[:, 0:HISTORY], series, (((1,), (0,)), ((), ())),
            precision=lax.Precision.HIGHEST, preferred_element_type=f32)

    staying = [filtered(jnp.concatenate([history_of(c, n) for n in range(1, 4)], axis=1)) for c in range(2)]
    keep_filtered(staying, slice(128, 512))

    for copy in edge_copies:
        copy.wait_recv()
    where_from = {move: j for j, move in enumerate(moves)}
    top = edges_in[where_from[(1, 0)]]
    bottom = edges_in[where_from[(-1, 0)]]
    left = edges_in[where_from[(0, 1)]]
    right = edges_in[where_from[(0, -1)]]
    top_left = edges_in[where_from[(1, 1)]][:, 127:128]
    top_right = edges_in[where_from[(1, -1)]][:, 0:1]
    bottom_left = edges_in[where_from[(-1, 1)]][:, 127:128]
    bottom_right = edges_in[where_from[(-1, -1)]][:, 0:1]

    def all_corners(section):
        step, part = section // 4, section % 4
        cell_y, cell_x = cell_of(section)
        sides = {}
        for dy in range(2):
            yy = cell_y + dy
            sides[dy] = (lookup(left, yy), lookup(right, yy))
        result = []
        ends = {}
        for dx in range(2):
            xx = cell_x + dx
            ends[dx] = tuple(
                jnp.where(xx < 0, lower, jnp.where(xx > 127, upper, lookup(line, xx)))
                for line, lower, upper in ((top, top_left, top_right), (bottom, bottom_left, bottom_right)))
        for dy in range(2):
            for dx in range(2):
                yy, xx = cell_y + dy, cell_x + dx
                outer = jnp.where(xx < 0, sides[dy][0], jnp.where(xx > 127, sides[dy][1], 0.0))
                outer = jnp.where(yy < 0, ends[dx][0], jnp.where(yy > 127, ends[dx][1], outer))
                rows = []
                for c in range(2):
                    a = step + (part == 3)
                    value = outer[3 * c + a : 3 * c + a + 1]
                    if part in (1, 2):
                        value = 0.5 * (value + outer[3 * c + a + 1 : 3 * c + a + 2])
                    rows.append(value)
                at = 4 * dy + 2 * dx
                result.append(corners[section, at : at + 2, :] + jnp.concatenate(rows, axis=0))
        return result

    def sample(section, held, point):
        cell_y, cell_x = cell_of(section)
        wy = point[0:1] - cell_y.astype(f32)
        wx = point[1:2] - cell_x.astype(f32)
        first_c, second_c, third_c, fourth_c = held
        return (1.0 - wy) * ((1.0 - wx) * first_c + wx * second_c) + wy * ((1.0 - wx) * third_c + wx * fourth_c)

    def rest_of_step(step, held, point, k_one):
        spot = point + 0.5 * drift * k_one
        k_two = sample(4 * step + 1, held[0], spot)
        spot = point + 0.5 * drift * k_two
        k_three = sample(4 * step + 2, held[1], spot)
        spot = point + drift * k_three
        k_four = sample(4 * step + 3, held[2], spot)
        return point + drift / 6.0 * (k_one + 2.0 * k_two + 2.0 * k_three + k_four)

    point = start_ref[...]
    k_first = sample(0, all_corners(0), point)
    point = rest_of_step(0, [all_corners(s) for s in (1, 2, 3)], point, k_first)

    spots[0:2, :] = point[:, 0:128]
    spots[2:4, :] = k_first[:, 0:128]
    spots[4:8, :] = jnp.zeros((4, 128), f32)
    for copy in spot_copies:
        copy.start()

    for copy in packed_copies:
        copy.wait_recv()
    lane = iota((1, 128), 1)
    changed = []
    for c in range(2):
        block = packed_in[:, :, 128 * c : 128 * c + HISTORY].reshape(128, HISTORY)
        high, low = halves(block)
        came = dot(high, leaving, TN) + dot(low, leaving, TN)
        changed.append(filtered(jnp.where(lane < starts[8], came, history_of(c, 0))))
    keep_filtered(changed, slice(0, 128))
    last_low = [jnp.concatenate([changed[c][72:73], staying[c][72:73]], axis=1) for c in range(2)]

    def deliver(k, carry):
        goal = lax.rem(ty + k, 8)
        pairs = dot(chosen[k], split_main[...], NT)
        message[pl.ds(16 * k, 16), 0:16, :] = (pairs[:, 0:128] + pairs[:, 128:256]).reshape(16, 16, 128)
        tail = dot(split_tail[...], chosen[k], NT)
        tail = tail[0:16] + tail[16:32]
        for h in range(2):
            for a in range(2):
                swapped = swap_blocks(tail[8 * a : 8 * a + 8, 128 * h : 128 * h + 128])
                message[pl.ds(16 * k + 8 * h, 8), 16 + a, :] = swapped

        def send(column):
            pltpu.make_async_remote_copy(
                src_ref=message.at[16 * k + column, pl.ds(0, EARLY)], dst_ref=arrived.at[me, pl.ds(0, EARLY)],
                send_sem=send_sem, recv_sem=recv_sem.at[k], device_id=(goal, column), device_id_type=MESH).start()

        for m in range(1, 16):
            send(along_x[m])

        @pl.when(k > 0)
        def _():
            send(tx)

        return carry

    lax.fori_loop(0, 8, deliver, 0)
    own_copy = pltpu.make_async_copy(message.at[tx, pl.ds(0, EARLY)], arrived.at[me, pl.ds(0, EARLY)], own_sems.at[0])
    own_copy.start()

    next_corners = all_corners(4)
    for copy in spot_copies:
        copy.wait_recv()
    moved_point = point[:, 0:128]
    moved_first = k_first[:, 0:128]
    for j in range(8):
        dy, dx = moves[j]
        here = (lane >= starts[j]) & (lane < starts[j + 1])
        arrival = spots_in[j]
        shift = jnp.where(iota((2, 128), 0) == 0, float(dy * 128), float(dx * 128))
        moved_point = jnp.where(here, arrival[0:2] - shift, moved_point)
        moved_first = jnp.where(here, arrival[2:4], moved_first)
    point = jnp.concatenate([moved_point, point[:, 128:512]], axis=1)
    k_first = jnp.concatenate([moved_first, k_first[:, 128:512]], axis=1)
    k_second = sample(4, next_corners, point)

    values = jnp.concatenate(last_low + [k_first, k_second, jnp.zeros((10, 512), f32)], axis=0)
    high, rest = halves(values)
    split_late[0:16, :] = high
    split_late[16:32, :] = rest

    def deliver_late(k, carry):
        goal = lax.rem(ty + k, 8)
        tail = dot(split_late[...], chosen[k], NT)
        tail = tail[0:8] + tail[16:24]
        for h in range(2):
            late[pl.ds(16 * k + 8 * h, 8), 0, :] = swap_blocks(tail[:, 128 * h : 128 * h + 128])

        def send(column):
            pltpu.make_async_remote_copy(
                src_ref=late.at[16 * k + column], dst_ref=late_in.at[me],
                send_sem=late_sems.at[0], recv_sem=late_sems.at[1], device_id=(goal, column),
                device_id_type=MESH).start()

        for m in range(1, 16):
            send(along_x[m])

        @pl.when(k > 0)
        def _():
            send(tx)

        return carry

    lax.fori_loop(0, 8, deliver_late, 0)
    own_late = pltpu.make_async_copy(late.at[tx], late_in.at[me], own_sems.at[1])
    own_late.start()

    end_ref[...] = rest_of_step(1, [all_corners(s) for s in (5, 6, 7)], point, k_second)

    def place_row(k, carry):
        sender = lax.rem(ty - k + 8, 8)

        @pl.when(k == 0)
        def _():
            landed = arrived.at[pl.ds(0, 15), pl.ds(0, EARLY)]
            pltpu.make_async_copy(landed, landed, recv_sem.at[0]).wait()
            own_copy.wait()

        @pl.when(k > 0)
        def _():
            landed = arrived.at[pl.ds(0, 16), pl.ds(0, EARLY)]
            pltpu.make_async_copy(landed, landed, recv_sem.at[k]).wait()

        slab = slabs.at[k]
        for h in range(2):
            tiles = pl.ds(sender * 16 + 8 * h, 8)
            wide = jnp.transpose(arrived[tiles, 0:16, :].reshape(128, 128))
            for c in range(2):
                slab[pl.ds(2 * h + c, 64, stride=4), :] = wide[64 * c : 64 * c + 64]
                slab[pl.ds(64 * 4 + 2 * h + c, 8, stride=4), :] = swap_blocks(arrived[tiles, 16 + c, :])
        pltpu.make_async_copy(slabs.at[k], slabs_ref.at[sender], slab_sems.at[k]).start()
        return carry

    lax.fori_loop(0, 8, place_row, 0)

    for copy in edge_copies + packed_copies + spot_copies:
        copy.wait_send()
    own_late.wait()
    sent = message.at[pl.ds(0, 127), pl.ds(0, EARLY)]
    pltpu.make_async_copy(sent, sent, send_sem).wait()
    sent = late.at[pl.ds(0, 127)]
    pltpu.make_async_copy(sent, sent, late_sems.at[0]).wait()
    pltpu.make_async_copy(sent, sent, late_sems.at[1]).wait()
    for block in range(16):
        part = swap_blocks(late_in[8 * block : 8 * block + 8, 0, :])
        for kind in range(3):
            late_ref[kind, 2 * block : 2 * block + 2, :] = part[2 * kind : 2 * kind + 2]
    for k in range(8):
        pltpu.make_async_copy(slabs.at[k], slabs_ref.at[lax.rem(ty - k + 8, 8)], slab_sems.at[k]).wait()


def finish_kernel(slabs_ref, late_ref, filter_ref, out_ref):
    rows = out_ref.reshape(SAMPLES * 8, 128)
    matrix = filter_ref[...]
    weights = [jnp.broadcast_to(matrix[:, at : at + 1], (SAMPLES, 128)) for at in (HISTORY, HISTORY + 1)]
    for s in range(2):
        for r in range(4):
            at = 4 * s + r
            early = slabs_ref[s, pl.ds(r, SAMPLES - 1, stride=4), :]
            low = jnp.concatenate([early, late_ref[0, at : at + 1, :]], axis=0)
            first, second = late_ref[1, at : at + 1, :], late_ref[2, at : at + 1, :]
            rows[pl.ds(at, SAMPLES, stride=8), :] = low + weights[0] * first + weights[1] * second


def per_device(velocity, start_position, cells, history, leavers, owner, filter_matrix):
    vmem = pl.BlockSpec(memory_space=pltpu.VMEM)
    hbm = pl.BlockSpec(memory_space=pl.ANY)
    slabs, late, end = pl.pallas_call(
        advance_kernel,
        out_shape=(
            jax.ShapeDtypeStruct((8, 288, 128), f32),
            jax.ShapeDtypeStruct((3, 32, 128), f32),
            jax.ShapeDtypeStruct((2, 512), f32),
        ),
        in_specs=[pl.BlockSpec(memory_space=pltpu.SMEM), hbm, vmem, vmem, hbm, vmem, vmem],
        out_specs=(hbm, vmem, vmem),
        scratch_shapes=[
            pltpu.VMEM((2, 3, 128, 128), f32),
            pltpu.VMEM((HISTORY * 8, 128), f32),
            pltpu.VMEM((5, 256, 256), bf16),
            pltpu.VMEM((4, 8, 128), f32),
            pltpu.VMEM((8, 8, 128), f32),
            pltpu.VMEM((8, 16, 256), f32),
            pltpu.VMEM((8, 16, 256), f32),
            pltpu.VMEM((8, 128), f32),
            pltpu.VMEM((8, 8, 128), f32),
            pltpu.VMEM((8, 8, 512), f32),
            pltpu.VMEM((8, 256, 512), bf16),
            pltpu.VMEM((256, 512), bf16),
            pltpu.VMEM((32, 512), bf16),
            pltpu.VMEM((32, 512), bf16),
            pltpu.VMEM((128, 24, 128), f32),
            pltpu.VMEM((128, 24, 128), f32),
            pltpu.VMEM((128, 1, 128), f32),
            pltpu.VMEM((128, 1, 128), f32),
            pltpu.VMEM((8, 288, 128), f32),
        ]
        + [pltpu.SemaphoreType.DMA((8,))] * 6
        + [
            pltpu.SemaphoreType.DMA,
            pltpu.SemaphoreType.DMA((8,)),
            pltpu.SemaphoreType.DMA((2,)),
            pltpu.SemaphoreType.DMA((2,)),
            pltpu.SemaphoreType.DMA((2,)),
            pltpu.SemaphoreType.DMA((8,)),
        ],
        compiler_params=pltpu.CompilerParams(collective_id=0, has_side_effects=True),
        name="advance",
    )(
        leavers, velocity, start_position, cells.reshape(8, 2, 512),
        history.reshape(2, HISTORY, 4, 128).transpose(1, 2, 0, 3).reshape(HISTORY * 8, 128),
        owner.reshape(1, 512), filter_matrix,
    )
    out = pl.pallas_call(
        finish_kernel,
        grid=(4,),
        out_shape=jax.ShapeDtypeStruct((SAMPLES, 32, 128), f32),
        in_specs=[
            pl.BlockSpec((2, 288, 128), lambda i: (i, 0, 0)),
            pl.BlockSpec((3, 8, 128), lambda i: (0, i, 0)),
            pl.BlockSpec((SAMPLES, SAMPLES), lambda i: (0, 0)),
        ],
        out_specs=pl.BlockSpec((SAMPLES, 8, 128), lambda i: (0, i, 0)),
        name="finish",
    )(slabs, late, filter_matrix)
    return out.reshape(SAMPLES, 16, 2, 128).transpose(2, 0, 1, 3).reshape(2, SAMPLES, 2048)


def solution(mesh):
    placed = (
        P(None, None, "ty", "tx"),
        P(None, ("ty", "tx")),
        P(None, None, None, ("ty", "tx")),
        P(None, None, ("ty", "tx")),
        P(),
        P(("ty", "tx"), None),
        P(),
    )
    return jax.shard_map(
        per_device,
        mesh=mesh,
        in_specs=placed,
        out_specs=P(None, None, ("ty", "tx")),
        check_vma=False,
    )
```

```python
import jax
import jax.numpy as jnp
from jax import lax
from jax.experimental import pallas as pl
from jax.experimental.pallas import tpu as pltpu
from jax.sharding import PartitionSpec as P

STEPS = 2
SAMPLES = 73
HISTORY = 71
MOST = 16
EARLY = 18
SPLIT = 6
STRIDE = 5

drift = 0.2
moves = ((-1, -1), (-1, 0), (-1, 1), (0, -1), (0, 1), (1, -1), (1, 0), (1, 1))
MESH = pl.DeviceIdType.MESH
f32 = jnp.float32
bf16 = jnp.bfloat16
i32 = jnp.int32
NT = (((1,), (1,)), ((), ()))
TN = (((0,), (0,)), ((), ()))


def iota(shape, dim):
    return lax.broadcasted_iota(i32, shape, dim)


def halves(x):
    high = x.astype(bf16)
    return high, (x - high.astype(f32)).astype(bf16)


def dot(a, b, dims=(((1,), (0,)), ((), ()))):
    return lax.dot_general(a, b, dims, preferred_element_type=f32)


def swap_blocks(x):
    sub = iota((8, 128), 0)
    block = iota((8, 128), 1) // 16
    for b in (1, 2, 4):
        row_bit = (sub // b) % 2
        col_bit = (block // b) % 2
        down = pltpu.roll(pltpu.roll(x, b, 0), 128 - 16 * b, 1)
        up = pltpu.roll(pltpu.roll(x, 8 - b, 0), 16 * b, 1)
        x = jnp.where(row_bit > col_bit, down, jnp.where(row_bit < col_bit, up, x))
    return x


def lookup(table, index):
    held = jnp.minimum(jnp.maximum(index, 0), 127)
    parts = []
    for n in range(4):
        at = jnp.broadcast_to(held[:, 128 * n : 128 * n + 128], (8, 128))
        parts.append(jnp.take_along_axis(table, at, axis=1))
    return jnp.concatenate(parts, axis=1)


def advance_kernel(
    leavers_ref, velocity_hbm, start_ref, cells_ref, history_hbm, owner_ref, filter_ref,
    slabs_ref, late_ref, end_ref,
    velocity_ref, history_ref, planes, edges, edges_in, packed, packed_in, spots, spots_in, corners,
    chosen, split_main, split_tail, split_late, message, arrived, late, late_in,
    edge_send, edge_recv, packed_send, packed_recv, spot_send, spot_recv, send_sems, recv_sem, late_sems, own_sems,
    input_sems, column_in,
):
    ty = lax.axis_index("ty")
    tx = lax.axis_index("tx")
    me = ty * 16 + tx
    down = [lax.rem(ty + k, 8) for k in range(8)]
    along_x = [lax.rem(tx + k, 16) for k in range(16)]
    barrier = pltpu.get_barrier_semaphore()
    load_velocity = pltpu.make_async_copy(velocity_hbm, velocity_ref, input_sems.at[0])
    load_history = pltpu.make_async_copy(history_hbm, history_ref, input_sems.at[1])
    load_velocity.start()
    load_history.start()

    close = [(0, m) for m in range(1, 16)] + [(k, 0) for k in range(1, 8)] + [(1, 1), (1, 15), (7, 1), (7, 15)]
    for k, m in close:
        pl.semaphore_signal(barrier, inc=1, device_id=(down[k], along_x[m]), device_id_type=MESH)

    def cell_of(section):
        both = cells_ref[section]
        return both[0:1], both[1:2]

    def neighbour(j):
        dy, dx = moves[j]
        return (down[dy % 8], along_x[dx % 16])

    def history_of(c, n):
        return history_ref[pl.ds(2 * n + c, HISTORY, stride=8), :]

    counts = [leavers_ref[0, j] for j in range(8)]
    starts = [0]
    for j in range(8):
        starts.append(starts[j] + counts[j])
    place = iota((128, 128), 0) % 16
    way = iota((128, 128), 0) // 16
    first = jnp.zeros((128, 128), i32)
    many = jnp.zeros((128, 128), i32)
    for j in range(8):
        first = jnp.where(way == j, starts[j], first)
        many = jnp.where(way == j, counts[j], many)
    leaving = (iota((128, 128), 1) == first + place) & (place < many)
    leaving = jnp.where(leaving, 1.0, 0.0).astype(bf16)

    load_velocity.wait()
    for a in range(3):
        for c in range(2):
            high, low = halves(velocity_ref[c, a])
            planes[2 * a, 128 * c : 128 * c + 128, 0:128] = high
            planes[2 * a, 128 * c : 128 * c + 128, 128:256] = low
    pick_row = iota((8, 256), 0)
    pick_lane = iota((8, 256), 1) % 128
    pick = ((pick_lane == 0) & (pick_row == 0)) | ((pick_lane == 127) & (pick_row == 1))
    pick = jnp.where(pick, 1.0, 0.0).astype(bf16)
    for a in range(3):
        sides = dot(pick, planes[2 * a], NT)
        for c in range(2):
            r = 3 * c + a
            edges[0, r : r + 1, :] = velocity_ref[c, a, 0:1, :]
            edges[1, r : r + 1, :] = velocity_ref[c, a, 127:128, :]
            edges[2, r : r + 1, :] = sides[0:1, 128 * c : 128 * c + 128]
            edges[3, r : r + 1, :] = sides[1:2, 128 * c : 128 * c + 128]
    for kind in range(4):
        edges[kind, 6:8, :] = jnp.zeros((2, 128), f32)

    load_history.wait()
    for c in range(2):
        high, low = halves(history_of(c, 0))
        block = dot(leaving, high, NT) + dot(leaving, low, NT)
        packed[:, :, 128 * c : 128 * c + HISTORY] = block.reshape(8, 16, HISTORY)

    for a in range(2):
        for c in range(2):
            high, low = halves(0.5 * (velocity_ref[c, a] + velocity_ref[c, a + 1]))
            planes[2 * a + 1, 128 * c : 128 * c + 128, 0:128] = high
            planes[2 * a + 1, 128 * c : 128 * c + 128, 128:256] = low

    def gather(section, carry):
        plane = planes[2 * (section // 4) + (section % 4 + 1) // 2]
        cell_y, cell_x = cell_of(section)
        column = iota((256, 512), 0) % 128
        row = iota((128, 512), 0)
        for dx in range(2):
            here = jnp.where(column == cell_x + dx, 1.0, 0.0).astype(bf16)
            along = dot(plane, here)
            for dy in range(2):
                on = row == cell_y + dy
                for c in range(2):
                    part = jnp.where(on, along[128 * c : 128 * c + 128], 0.0)
                    at = 4 * dy + 2 * dx + c
                    corners[section, at : at + 1, :] = jnp.sum(part, axis=0, keepdims=True)
        return carry

    lax.fori_loop(0, 4, gather, 0)

    pl.semaphore_wait(barrier, len(close))
    for m in range(1, 16):
        pl.semaphore_signal(column_in, inc=1, device_id=(ty, along_x[m]), device_id_type=MESH)

    edge_copies = []
    packed_copies = []
    spot_copies = []
    for j in range(8):
        dy, dx = moves[j]
        kind = {1: 1, -1: 0}.get(dy, 3 if dx == 1 else 2)
        edge_copies.append(pltpu.make_async_remote_copy(
            src_ref=edges.at[kind], dst_ref=edges_in.at[j], send_sem=edge_send.at[j], recv_sem=edge_recv.at[j],
            device_id=neighbour(j), device_id_type=MESH))
        packed_copies.append(pltpu.make_async_remote_copy(
            src_ref=packed.at[j], dst_ref=packed_in.at[j], send_sem=packed_send.at[j], recv_sem=packed_recv.at[j],
            device_id=neighbour(j), device_id_type=MESH))
        spot_copies.append(pltpu.make_async_remote_copy(
            src_ref=spots, dst_ref=spots_in.at[j], send_sem=spot_send.at[j], recv_sem=spot_recv.at[j],
            device_id=neighbour(j), device_id_type=MESH))
    for copy in edge_copies:
        copy.start()
    for copy in packed_copies:
        copy.start()

    named = iota((128, 512), 0) == owner_ref[...]
    before = dot(
        jnp.where(named, 1.0, 0.0).astype(bf16),
        jnp.where(iota((512, 512), 0) < iota((512, 512), 1), 1.0, 0.0).astype(bf16))
    rank = jnp.sum(jnp.where(named, before, 0.0), axis=0, keepdims=True).astype(i32)
    target = owner_ref[...] * 16 + rank

    matrix = filter_ref[...]

    def keep_filtered(low, lanes):
        for c in range(2):
            high, rest = halves(low[c][0:64])
            split_main[64 * c : 64 * c + 64, lanes] = high
            split_main[128 + 64 * c : 192 + 64 * c, lanes] = rest
        high, rest = halves(jnp.concatenate([low[0][64:72], low[1][64:72]], axis=0))
        split_tail[0:16, lanes] = high
        split_tail[16:32, lanes] = rest

    def filtered(series):
        return lax.dot_general(
            matrix[:, 0:HISTORY], series, (((1,), (0,)), ((), ())),
            precision=lax.Precision.HIGHEST, preferred_element_type=f32)

    staying = [filtered(jnp.concatenate([history_of(c, n) for n in range(1, 4)], axis=1)) for c in range(2)]
    keep_filtered(staying, slice(128, 512))

    for copy in edge_copies:
        copy.wait_recv()
    where_from = {move: j for j, move in enumerate(moves)}
    top = edges_in[where_from[(1, 0)]]
    bottom = edges_in[where_from[(-1, 0)]]
    left = edges_in[where_from[(0, 1)]]
    right = edges_in[where_from[(0, -1)]]
    top_left = edges_in[where_from[(1, 1)]][:, 127:128]
    top_right = edges_in[where_from[(1, -1)]][:, 0:1]
    bottom_left = edges_in[where_from[(-1, 1)]][:, 127:128]
    bottom_right = edges_in[where_from[(-1, -1)]][:, 0:1]

    def all_corners(section):
        step, part = section // 4, section % 4
        cell_y, cell_x = cell_of(section)
        sides = {}
        for dy in range(2):
            yy = cell_y + dy
            sides[dy] = (lookup(left, yy), lookup(right, yy))
        result = []
        ends = {}
        for dx in range(2):
            xx = cell_x + dx
            ends[dx] = tuple(
                jnp.where(xx < 0, lower, jnp.where(xx > 127, upper, lookup(line, xx)))
                for line, lower, upper in ((top, top_left, top_right), (bottom, bottom_left, bottom_right)))
        for dy in range(2):
            for dx in range(2):
                yy, xx = cell_y + dy, cell_x + dx
                outer = jnp.where(xx < 0, sides[dy][0], jnp.where(xx > 127, sides[dy][1], 0.0))
                outer = jnp.where(yy < 0, ends[dx][0], jnp.where(yy > 127, ends[dx][1], outer))
                rows = []
                for c in range(2):
                    a = step + (part == 3)
                    value = outer[3 * c + a : 3 * c + a + 1]
                    if part in (1, 2):
                        value = 0.5 * (value + outer[3 * c + a + 1 : 3 * c + a + 2])
                    rows.append(value)
                at = 4 * dy + 2 * dx
                result.append(corners[section, at : at + 2, :] + jnp.concatenate(rows, axis=0))
        return result

    def sample(section, held, point):
        cell_y, cell_x = cell_of(section)
        wy = point[0:1] - cell_y.astype(f32)
        wx = point[1:2] - cell_x.astype(f32)
        first_c, second_c, third_c, fourth_c = held
        return (1.0 - wy) * ((1.0 - wx) * first_c + wx * second_c) + wy * ((1.0 - wx) * third_c + wx * fourth_c)

    def rest_of_step(step, held, point, k_one):
        spot = point + 0.5 * drift * k_one
        k_two = sample(4 * step + 1, held[0], spot)
        spot = point + 0.5 * drift * k_two
        k_three = sample(4 * step + 2, held[1], spot)
        spot = point + drift * k_three
        k_four = sample(4 * step + 3, held[2], spot)
        return point + drift / 6.0 * (k_one + 2.0 * k_two + 2.0 * k_three + k_four)

    point = start_ref[...]
    k_first = sample(0, all_corners(0), point)
    point = rest_of_step(0, [all_corners(s) for s in (1, 2, 3)], point, k_first)

    spots[0:2, :] = point[:, 0:128]
    spots[2:4, :] = k_first[:, 0:128]
    spots[4:8, :] = jnp.zeros((4, 128), f32)
    for copy in spot_copies:
        copy.start()

    for copy in packed_copies:
        copy.wait_recv()
    lane = iota((1, 128), 1)
    changed = []
    for c in range(2):
        block = packed_in[:, :, 128 * c : 128 * c + HISTORY].reshape(128, HISTORY)
        high, low = halves(block)
        came = dot(high, leaving, TN) + dot(low, leaving, TN)
        changed.append(filtered(jnp.where(lane < starts[8], came, history_of(c, 0))))
    keep_filtered(changed, slice(0, 128))
    last_low = [jnp.concatenate([changed[c][72:73], staying[c][72:73]], axis=1) for c in range(2)]

    def fill(k):
        place = target - lax.rem(ty + STRIDE * k, 8) * 256
        here = jnp.where(iota((256, 512), 0) == place, 1.0, 0.0).astype(bf16)
        pairs = dot(here, split_main[...], NT)
        message[pl.ds(16 * k, 16), 0:16, :] = (pairs[:, 0:128] + pairs[:, 128:256]).reshape(16, 16, 128)
        tail = dot(split_tail[...], here, NT)
        tail = tail[0:16] + tail[16:32]
        for h in range(2):
            for a in range(2):
                swapped = swap_blocks(tail[8 * a : 8 * a + 8, 128 * h : 128 * h + 128])
                message[pl.ds(16 * k + 8 * h, 8), 16 + a, :] = swapped
        return here

    def newest(here):
        tail = dot(split_late[...], here, NT)
        tail = tail[0:8] + tail[16:24]
        return [swap_blocks(tail[:, 128 * h : 128 * h + 128]) for h in range(2)]

    def send_row(k, copy_to):
        goal = lax.rem(ty + STRIDE * k, 8)
        for m in range(1, 16):
            copy_to(goal, along_x[m]).start()

        @pl.when(k > 0)
        def _():
            copy_to(goal, tx).start()

    def bulk(k, rows):
        def copy_to(goal, column):
            return pltpu.make_async_remote_copy(
                src_ref=message.at[16 * k + column, pl.ds(0, rows)], dst_ref=arrived.at[me, pl.ds(0, rows)],
                send_sem=send_sems.at[rows - EARLY], recv_sem=recv_sem.at[k], device_id=(goal, column),
                device_id_type=MESH)

        return copy_to

    def deliver(k, carry):
        chosen[k] = fill(k)
        send_row(k, bulk(k, EARLY))
        return carry

    pl.semaphore_wait(column_in, 15)
    lax.fori_loop(0, SPLIT, deliver, 0)
    own_copy = pltpu.make_async_copy(message.at[tx, pl.ds(0, EARLY)], arrived.at[me, pl.ds(0, EARLY)], own_sems.at[0])
    own_copy.start()

    lax.fori_loop(4, 8, gather, 0)
    next_corners = all_corners(4)
    for copy in spot_copies:
        copy.wait_recv()
    moved_point = point[:, 0:128]
    moved_first = k_first[:, 0:128]
    for j in range(8):
        dy, dx = moves[j]
        here = (lane >= starts[j]) & (lane < starts[j + 1])
        arrival = spots_in[j]
        shift = jnp.where(iota((2, 128), 0) == 0, float(dy * 128), float(dx * 128))
        moved_point = jnp.where(here, arrival[0:2] - shift, moved_point)
        moved_first = jnp.where(here, arrival[2:4], moved_first)
    point = jnp.concatenate([moved_point, point[:, 128:512]], axis=1)
    k_first = jnp.concatenate([moved_first, k_first[:, 128:512]], axis=1)
    k_second = sample(4, next_corners, point)

    values = jnp.concatenate(last_low + [k_first, k_second, jnp.zeros((10, 512), f32)], axis=0)
    high, rest = halves(values)
    split_late[0:16, :] = high
    split_late[16:32, :] = rest

    def deliver_late(k, carry):
        parts = newest(chosen[k])
        for h in range(2):
            late[pl.ds(16 * k + 8 * h, 8), 0, :] = parts[h]

        def copy_to(goal, column):
            return pltpu.make_async_remote_copy(
                src_ref=late.at[16 * k + column], dst_ref=late_in.at[me], send_sem=late_sems.at[0],
                recv_sem=late_sems.at[1], device_id=(goal, column), device_id_type=MESH)

        send_row(k, copy_to)
        return carry

    lax.fori_loop(0, SPLIT, deliver_late, 0)

    def deliver_all(k, carry):
        parts = newest(fill(k))
        for h in range(2):
            message[pl.ds(16 * k + 8 * h, 8), EARLY, :] = parts[h]
        send_row(k, bulk(k, EARLY + 1))
        return carry

    lax.fori_loop(SPLIT, 8, deliver_all, 0)
    own_late = pltpu.make_async_copy(late.at[tx], late_in.at[me], own_sems.at[1])
    own_late.start()

    end_ref[...] = rest_of_step(1, [all_corners(s) for s in (5, 6, 7)], point, k_second)

    def landed(number, rows):
        return arrived.at[pl.ds(0, number), pl.ds(0, rows)]

    def keep_late(sender, h, part):
        part = swap_blocks(part)
        for kind in range(3):
            late_ref[kind, sender, 2 * h : 2 * h + 2, :] = part[2 * kind : 2 * kind + 2]

    def place_row(k, carry):
        sender = lax.rem(ty - STRIDE * k + 64, 8)

        @pl.when(k == 0)
        def _():
            pltpu.make_async_copy(landed(15, EARLY), landed(15, EARLY), recv_sem.at[0]).wait()
            own_copy.wait()

        @pl.when((k > 0) & (k < SPLIT))
        def _():
            pltpu.make_async_copy(landed(16, EARLY), landed(16, EARLY), recv_sem.at[k]).wait()

        @pl.when(k >= SPLIT)
        def _():
            pltpu.make_async_copy(landed(16, EARLY + 1), landed(16, EARLY + 1), recv_sem.at[k]).wait()
            for h in range(2):
                keep_late(sender, h, arrived[pl.ds(sender * 16 + 8 * h, 8), EARLY, :])

        slab = slabs_ref.at[sender]
        for h in range(2):
            tiles = pl.ds(sender * 16 + 8 * h, 8)
            wide = jnp.transpose(arrived[tiles, 0:16, :].reshape(128, 128))
            for c in range(2):
                slab[pl.ds(2 * h + c, 64, stride=4), :] = wide[64 * c : 64 * c + 64]
                slab[pl.ds(64 * 4 + 2 * h + c, 8, stride=4), :] = swap_blocks(arrived[tiles, 16 + c, :])
        return carry

    lax.fori_loop(0, 8, place_row, 0)

    own_late.wait()
    few = 16 * SPLIT - 1
    sent = late.at[pl.ds(0, few)]
    pltpu.make_async_copy(sent, sent, late_sems.at[1]).wait()
    for k in range(SPLIT):
        sender = lax.rem(ty - STRIDE * k + 64, 8)
        for h in range(2):
            keep_late(sender, h, late_in[pl.ds(sender * 16 + 8 * h, 8), 0, :])
    for copy in edge_copies + packed_copies + spot_copies:
        copy.wait_send()
    pltpu.make_async_copy(sent, sent, late_sems.at[0]).wait()
    pltpu.make_async_copy(landed(few, EARLY), landed(few, EARLY), send_sems.at[0]).wait()
    rest = 128 - 16 * SPLIT
    pltpu.make_async_copy(landed(rest, EARLY + 1), landed(rest, EARLY + 1), send_sems.at[1]).wait()


def finish_kernel(slabs_ref, late_ref, filter_ref, out_ref, buffer, sems):
    matrix = filter_ref[...]
    weights = [jnp.broadcast_to(matrix[:, at : at + 1], (SAMPLES, 128)) for at in (HISTORY, HISTORY + 1)]
    copies = []
    for part in range(4):
        rows = buffer.at[part].reshape(SAMPLES * 8, 128)
        for r in range(8):
            at = 8 * part + r
            early = slabs_ref[at // 4, pl.ds(at % 4, SAMPLES - 1, stride=4), :]
            low = jnp.concatenate([early, late_ref[0, at // 4, at % 4 : at % 4 + 1, :]], axis=0)
            first, second = (late_ref[kind, at // 4, at % 4 : at % 4 + 1, :] for kind in (1, 2))
            rows[pl.ds(r, SAMPLES, stride=8), :] = low + weights[0] * first + weights[1] * second
        copies.append(pltpu.make_async_copy(buffer.at[part], out_ref.at[:, pl.ds(8 * part, 8), :], sems.at[part]))
        copies[-1].start()
    for copy in copies:
        copy.wait()


def per_device(velocity, start_position, cells, history, leavers, owner, filter_matrix):
    vmem = pl.BlockSpec(memory_space=pltpu.VMEM)
    hbm = pl.BlockSpec(memory_space=pl.ANY)
    slabs, late, end = pl.pallas_call(
        advance_kernel,
        out_shape=(
            pltpu.VMEM((8, 288, 128), f32),
            pltpu.VMEM((3, 8, 4, 128), f32),
            jax.ShapeDtypeStruct((2, 512), f32),
        ),
        in_specs=[pl.BlockSpec(memory_space=pltpu.SMEM), hbm, vmem, vmem, hbm, vmem, vmem],
        out_specs=(vmem, vmem, vmem),
        scratch_shapes=[
            pltpu.VMEM((2, 3, 128, 128), f32),
            pltpu.VMEM((HISTORY * 8, 128), f32),
            pltpu.VMEM((5, 256, 256), bf16),
            pltpu.VMEM((4, 8, 128), f32),
            pltpu.VMEM((8, 8, 128), f32),
            pltpu.VMEM((8, 16, 256), f32),
            pltpu.VMEM((8, 16, 256), f32),
            pltpu.VMEM((8, 128), f32),
            pltpu.VMEM((8, 8, 128), f32),
            pltpu.VMEM((8, 8, 512), f32),
            pltpu.VMEM((SPLIT, 256, 512), bf16),
            pltpu.VMEM((256, 512), bf16),
            pltpu.VMEM((32, 512), bf16),
            pltpu.VMEM((32, 512), bf16),
            pltpu.VMEM((128, 24, 128), f32),
            pltpu.VMEM((128, 24, 128), f32),
            pltpu.VMEM((16 * SPLIT, 1, 128), f32),
            pltpu.VMEM((128, 1, 128), f32),
        ]
        + [pltpu.SemaphoreType.DMA((8,))] * 6
        + [
            pltpu.SemaphoreType.DMA((2,)),
            pltpu.SemaphoreType.DMA((8,)),
            pltpu.SemaphoreType.DMA((2,)),
            pltpu.SemaphoreType.DMA((2,)),
            pltpu.SemaphoreType.DMA((2,)),
            pltpu.SemaphoreType.REGULAR,
        ],
        compiler_params=pltpu.CompilerParams(collective_id=0, has_side_effects=True),
        name="advance",
    )(
        leavers, velocity, start_position, cells.reshape(8, 2, 512),
        history.reshape(2, HISTORY, 4, 128).transpose(1, 2, 0, 3).reshape(HISTORY * 8, 128),
        owner.reshape(1, 512), filter_matrix,
    )
    out = pl.pallas_call(
        finish_kernel,
        out_shape=jax.ShapeDtypeStruct((SAMPLES, 32, 128), f32),
        in_specs=[vmem, vmem, vmem],
        out_specs=hbm,
        scratch_shapes=[pltpu.VMEM((4, SAMPLES, 8, 128), f32), pltpu.SemaphoreType.DMA((4,))],
        name="finish",
    )(
        pltpu.with_memory_space_constraint(slabs, pltpu.VMEM),
        pltpu.with_memory_space_constraint(late, pltpu.VMEM),
        filter_matrix,
    )
    return out.reshape(SAMPLES, 16, 2, 128).transpose(2, 0, 1, 3).reshape(2, SAMPLES, 2048)


def solution(mesh):
    placed = (
        P(None, None, "ty", "tx"),
        P(None, ("ty", "tx")),
        P(None, None, None, ("ty", "tx")),
        P(None, None, ("ty", "tx")),
        P(),
        P(("ty", "tx"), None),
        P(),
    )
    return jax.shard_map(
        per_device,
        mesh=mesh,
        in_specs=placed,
        out_specs=P(None, None, ("ty", "tx")),
        check_vma=False,
    )
```

```python
import jax
import jax.numpy as jnp
from jax import lax
from jax.experimental import pallas as pl
from jax.experimental.pallas import tpu as pltpu
from jax.sharding import PartitionSpec as P

STEPS = 2
SAMPLES = 73
HISTORY = 71
MOST = 16
EARLY = 18
SPLIT = 6
drift = 0.2
moves = ((-1, -1), (-1, 0), (-1, 1), (0, -1), (0, 1), (1, -1), (1, 0), (1, 1))
MESH = pl.DeviceIdType.MESH
f32 = jnp.float32
bf16 = jnp.bfloat16
i32 = jnp.int32
NT = (((1,), (1,)), ((), ()))
TN = (((0,), (0,)), ((), ()))


def iota(shape, dim):
    return lax.broadcasted_iota(i32, shape, dim)


def halves(x):
    high = x.astype(bf16)
    return high, (x - high.astype(f32)).astype(bf16)


def dot(a, b, dims=(((1,), (0,)), ((), ()))):
    return lax.dot_general(a, b, dims, preferred_element_type=f32)


def offset(k):
    if isinstance(k, int):
        return 5 * k % 8
    return lax.rem(5 * k, 8)


def swap_blocks(x):
    sub = iota((8, 128), 0)
    block = iota((8, 128), 1) // 16
    for b in (1, 2, 4):
        row_bit = (sub // b) % 2
        col_bit = (block // b) % 2
        down = pltpu.roll(pltpu.roll(x, b, 0), 128 - 16 * b, 1)
        up = pltpu.roll(pltpu.roll(x, 8 - b, 0), 16 * b, 1)
        x = jnp.where(row_bit > col_bit, down, jnp.where(row_bit < col_bit, up, x))
    return x


def lookup(table, index):
    held = jnp.minimum(jnp.maximum(index, 0), 127)
    parts = []
    for n in range(4):
        at = jnp.broadcast_to(held[:, 128 * n : 128 * n + 128], (8, 128))
        parts.append(jnp.take_along_axis(table, at, axis=1))
    return jnp.concatenate(parts, axis=1)


def advance_kernel(
    leavers_ref, velocity_hbm, start_ref, cells_ref, history_hbm, owner_ref, filter_ref,
    slabs_ref, late_ref, end_ref,
    velocity_ref, history_ref, planes, edges, edges_in, packed, packed_in, spots, spots_in, corners,
    chosen, standing, split_main, split_tail, split_late, message, arrived, late, late_in,
    edge_send, edge_recv, packed_send, packed_recv, spot_send, spot_recv, send_sems, recv_sem, late_sems, own_sems,
    input_sems, column_in,
):
    ty = lax.axis_index("ty")
    tx = lax.axis_index("tx")
    me = ty * 16 + tx
    down = [lax.rem(ty + k, 8) for k in range(8)]
    along_x = [lax.rem(tx + k, 16) for k in range(16)]
    barrier = pltpu.get_barrier_semaphore()
    load_velocity = pltpu.make_async_copy(velocity_hbm, velocity_ref, input_sems.at[0])
    load_history = pltpu.make_async_copy(history_hbm, history_ref, input_sems.at[1])
    load_velocity.start()
    load_history.start()

    close = [(0, m) for m in range(1, 16)] + [(k, 0) for k in range(1, 8)] + [(1, 1), (1, 15), (7, 1), (7, 15)]
    for k, m in close:
        pl.semaphore_signal(barrier, inc=1, device_id=(down[k], along_x[m]), device_id_type=MESH)

    def cell_of(section):
        both = cells_ref[section]
        return both[0:1], both[1:2]

    def neighbour(j):
        dy, dx = moves[j]
        return (down[dy % 8], along_x[dx % 16])

    def history_of(c, n):
        return history_ref[pl.ds(2 * n + c, HISTORY, stride=8), :]

    counts = [leavers_ref[0, j] for j in range(8)]
    starts = [0]
    for j in range(8):
        starts.append(starts[j] + counts[j])
    place = iota((128, 128), 0) % 16
    way = iota((128, 128), 0) // 16
    first = jnp.zeros((128, 128), i32)
    many = jnp.zeros((128, 128), i32)
    for j in range(8):
        first = jnp.where(way == j, starts[j], first)
        many = jnp.where(way == j, counts[j], many)
    leaving = (iota((128, 128), 1) == first + place) & (place < many)
    leaving = jnp.where(leaving, 1.0, 0.0).astype(bf16)

    load_velocity.wait()
    for a in range(3):
        for c in range(2):
            high, low = halves(velocity_ref[c, a])
            planes[2 * a, 128 * c : 128 * c + 128, 0:128] = high
            planes[2 * a, 128 * c : 128 * c + 128, 128:256] = low
    pick_row = iota((8, 256), 0)
    pick_lane = iota((8, 256), 1) % 128
    pick = ((pick_lane == 0) & (pick_row == 0)) | ((pick_lane == 127) & (pick_row == 1))
    pick = jnp.where(pick, 1.0, 0.0).astype(bf16)
    for a in range(3):
        sides = dot(pick, planes[2 * a], NT)
        for c in range(2):
            r = 3 * c + a
            edges[0, r : r + 1, :] = velocity_ref[c, a, 0:1, :]
            edges[1, r : r + 1, :] = velocity_ref[c, a, 127:128, :]
            edges[2, r : r + 1, :] = sides[0:1, 128 * c : 128 * c + 128]
            edges[3, r : r + 1, :] = sides[1:2, 128 * c : 128 * c + 128]
    for kind in range(4):
        edges[kind, 6:8, :] = jnp.zeros((2, 128), f32)

    load_history.wait()
    for c in range(2):
        high, low = halves(history_of(c, 0))
        block = dot(leaving, high, NT) + dot(leaving, low, NT)
        packed[:, :, 128 * c : 128 * c + HISTORY] = block.reshape(8, 16, HISTORY)

    for a in range(2):
        for c in range(2):
            high, low = halves(0.5 * (velocity_ref[c, a] + velocity_ref[c, a + 1]))
            planes[2 * a + 1, 128 * c : 128 * c + 128, 0:128] = high
            planes[2 * a + 1, 128 * c : 128 * c + 128, 128:256] = low

    def gather(section, carry):
        plane = planes[2 * (section // 4) + (section % 4 + 1) // 2]
        cell_y, cell_x = cell_of(section)
        column = iota((256, 512), 0) % 128
        row = iota((128, 512), 0)
        for dx in range(2):
            here = jnp.where(column == cell_x + dx, 1.0, 0.0).astype(bf16)
            along = dot(plane, here)
            for dy in range(2):
                on = row == cell_y + dy
                for c in range(2):
                    part = jnp.where(on, along[128 * c : 128 * c + 128], 0.0)
                    at = 4 * dy + 2 * dx + c
                    corners[section, at : at + 1, :] = jnp.sum(part, axis=0, keepdims=True)
        return carry

    lax.fori_loop(0, 4, gather, 0)

    pl.semaphore_wait(barrier, len(close))
    for m in range(1, 16):
        pl.semaphore_signal(column_in, inc=1, device_id=(ty, along_x[m]), device_id_type=MESH)

    edge_copies = []
    packed_copies = []
    spot_copies = []
    for j in range(8):
        dy, dx = moves[j]
        kind = {1: 1, -1: 0}.get(dy, 3 if dx == 1 else 2)
        edge_copies.append(pltpu.make_async_remote_copy(
            src_ref=edges.at[kind], dst_ref=edges_in.at[j], send_sem=edge_send.at[j], recv_sem=edge_recv.at[j],
            device_id=neighbour(j), device_id_type=MESH))
        packed_copies.append(pltpu.make_async_remote_copy(
            src_ref=packed.at[j], dst_ref=packed_in.at[j], send_sem=packed_send.at[j], recv_sem=packed_recv.at[j],
            device_id=neighbour(j), device_id_type=MESH))
        spot_copies.append(pltpu.make_async_remote_copy(
            src_ref=spots, dst_ref=spots_in.at[j], send_sem=spot_send.at[j], recv_sem=spot_recv.at[j],
            device_id=neighbour(j), device_id_type=MESH))
    for copy in edge_copies:
        copy.start()
    for copy in packed_copies:
        copy.start()

    named = iota((128, 512), 0) == owner_ref[...]
    before = dot(
        jnp.where(named, 1.0, 0.0).astype(bf16),
        jnp.where(iota((512, 512), 0) < iota((512, 512), 1), 1.0, 0.0).astype(bf16))
    rank = jnp.sum(jnp.where(named, before, 0.0), axis=0, keepdims=True).astype(i32)
    target = owner_ref[...] * 16 + rank
    for n in range(4):
        spread = jnp.broadcast_to(target[:, 128 * n : 128 * n + 128].astype(f32), (128, 128))
        standing[128 * n : 128 * n + 128, :] = jnp.transpose(spread).astype(i32)

    matrix = filter_ref[...]

    def keep_filtered(low, lanes):
        main = jnp.concatenate([low[0][0:64], low[1][0:64]], axis=0)
        for n in range(main.shape[1] // 128):
            at = lanes.start + 128 * n
            high, rest = halves(jnp.transpose(main[:, 128 * n : 128 * n + 128]))
            split_main[at : at + 128, 0:128] = high
            split_main[at : at + 128, 128:256] = rest
        high, rest = halves(jnp.concatenate([low[0][64:72], low[1][64:72]], axis=0))
        split_tail[0:16, lanes] = high
        split_tail[16:32, lanes] = rest

    def filtered(series):
        return lax.dot_general(
            matrix[:, 0:HISTORY], series, (((1,), (0,)), ((), ())),
            precision=lax.Precision.HIGHEST, preferred_element_type=f32)

    staying = [filtered(jnp.concatenate([history_of(c, n) for n in range(1, 4)], axis=1)) for c in range(2)]
    keep_filtered(staying, slice(128, 512))

    for copy in edge_copies:
        copy.wait_recv()
    where_from = {move: j for j, move in enumerate(moves)}
    top = edges_in[where_from[(1, 0)]]
    bottom = edges_in[where_from[(-1, 0)]]
    left = edges_in[where_from[(0, 1)]]
    right = edges_in[where_from[(0, -1)]]
    top_left = edges_in[where_from[(1, 1)]][:, 127:128]
    top_right = edges_in[where_from[(1, -1)]][:, 0:1]
    bottom_left = edges_in[where_from[(-1, 1)]][:, 127:128]
    bottom_right = edges_in[where_from[(-1, -1)]][:, 0:1]

    def all_corners(section):
        step, part = section // 4, section % 4
        cell_y, cell_x = cell_of(section)
        sides = {}
        for dy in range(2):
            yy = cell_y + dy
            sides[dy] = (lookup(left, yy), lookup(right, yy))
        result = []
        ends = {}
        for dx in range(2):
            xx = cell_x + dx
            ends[dx] = tuple(
                jnp.where(xx < 0, lower, jnp.where(xx > 127, upper, lookup(line, xx)))
                for line, lower, upper in ((top, top_left, top_right), (bottom, bottom_left, bottom_right)))
        for dy in range(2):
            for dx in range(2):
                yy, xx = cell_y + dy, cell_x + dx
                outer = jnp.where(xx < 0, sides[dy][0], jnp.where(xx > 127, sides[dy][1], 0.0))
                outer = jnp.where(yy < 0, ends[dx][0], jnp.where(yy > 127, ends[dx][1], outer))
                rows = []
                for c in range(2):
                    a = step + (part == 3)
                    value = outer[3 * c + a : 3 * c + a + 1]
                    if part in (1, 2):
                        value = 0.5 * (value + outer[3 * c + a + 1 : 3 * c + a + 2])
                    rows.append(value)
                at = 4 * dy + 2 * dx
                result.append(corners[section, at : at + 2, :] + jnp.concatenate(rows, axis=0))
        return result

    def sample(section, held, point):
        cell_y, cell_x = cell_of(section)
        wy = point[0:1] - cell_y.astype(f32)
        wx = point[1:2] - cell_x.astype(f32)
        first_c, second_c, third_c, fourth_c = held
        return (1.0 - wy) * ((1.0 - wx) * first_c + wx * second_c) + wy * ((1.0 - wx) * third_c + wx * fourth_c)

    def rest_of_step(step, held, point, k_one):
        spot = point + 0.5 * drift * k_one
        k_two = sample(4 * step + 1, held[0], spot)
        spot = point + 0.5 * drift * k_two
        k_three = sample(4 * step + 2, held[1], spot)
        spot = point + drift * k_three
        k_four = sample(4 * step + 3, held[2], spot)
        return point + drift / 6.0 * (k_one + 2.0 * k_two + 2.0 * k_three + k_four)

    point = start_ref[...]
    k_first = sample(0, all_corners(0), point)
    point = rest_of_step(0, [all_corners(s) for s in (1, 2, 3)], point, k_first)

    spots[0:2, :] = point[:, 0:128]
    spots[2:4, :] = k_first[:, 0:128]
    spots[4:8, :] = jnp.zeros((4, 128), f32)
    for copy in spot_copies:
        copy.start()

    for copy in packed_copies:
        copy.wait_recv()
    lane = iota((1, 128), 1)
    changed = []
    for c in range(2):
        block = packed_in[:, :, 128 * c : 128 * c + HISTORY].reshape(128, HISTORY)
        high, low = halves(block)
        came = dot(high, leaving, TN) + dot(low, leaving, TN)
        changed.append(filtered(jnp.where(lane < starts[8], came, history_of(c, 0))))
    keep_filtered(changed, slice(0, 128))
    last_low = [jnp.concatenate([changed[c][72:73], staying[c][72:73]], axis=1) for c in range(2)]

    def goal_of(k):
        return lax.rem(ty + offset(k), 8)

    def fill(k):
        first_column = goal_of(k) * 256
        here = jnp.where(iota((256, 512), 0) == target - first_column, 1.0, 0.0).astype(bf16)
        away = standing[...] - first_column
        across = jnp.concatenate(
            [jnp.where(iota((512, 128), 1) == away - 128 * h, 1.0, 0.0) for h in range(2)], axis=1).astype(bf16)
        pairs = dot(here, split_main[...])
        message[pl.ds(16 * k, 16), 0:16, :] = (pairs[:, 0:128] + pairs[:, 128:256]).reshape(16, 16, 128)
        tail = dot(split_tail[...], across)
        tail = tail[0:16] + tail[16:32]
        for h in range(2):
            for a in range(2):
                swapped = swap_blocks(tail[8 * a : 8 * a + 8, 128 * h : 128 * h + 128])
                message[pl.ds(16 * k + 8 * h, 8), 16 + a, :] = swapped
        return across

    def newest(across):
        tail = dot(split_late[...], across)
        tail = tail[0:8] + tail[16:24]
        return [swap_blocks(tail[:, 128 * h : 128 * h + 128]) for h in range(2)]

    def send_rows(rows, copy_of):
        for m in range(1, 16):
            for k in rows:
                copy_of(k, along_x[m]).start()
        for k in rows:
            @pl.when(k > 0)
            def _():
                copy_of(k, tx).start()

    def bulk(count):
        def copy_of(k, column):
            return pltpu.make_async_remote_copy(
                src_ref=message.at[16 * k + column, pl.ds(0, count)], dst_ref=arrived.at[me, pl.ds(0, count)],
                send_sem=send_sems.at[count - EARLY], recv_sem=recv_sem.at[k], device_id=(goal_of(k), column),
                device_id_type=MESH)

        return copy_of

    def deliver(pair, carry):
        rows = (2 * pair, 2 * pair + 1)
        for k in rows:
            chosen[k] = fill(k)
        send_rows(rows, bulk(EARLY))
        return carry

    pl.semaphore_wait(column_in, 15)
    lax.fori_loop(0, SPLIT // 2, deliver, 0)
    own_copy = pltpu.make_async_copy(message.at[tx, pl.ds(0, EARLY)], arrived.at[me, pl.ds(0, EARLY)], own_sems.at[0])
    own_copy.start()

    lax.fori_loop(4, 8, gather, 0)
    next_corners = all_corners(4)
    for copy in spot_copies:
        copy.wait_recv()
    moved_point = point[:, 0:128]
    moved_first = k_first[:, 0:128]
    for j in range(8):
        dy, dx = moves[j]
        here = (lane >= starts[j]) & (lane < starts[j + 1])
        arrival = spots_in[j]
        shift = jnp.where(iota((2, 128), 0) == 0, float(dy * 128), float(dx * 128))
        moved_point = jnp.where(here, arrival[0:2] - shift, moved_point)
        moved_first = jnp.where(here, arrival[2:4], moved_first)
    point = jnp.concatenate([moved_point, point[:, 128:512]], axis=1)
    k_first = jnp.concatenate([moved_first, k_first[:, 128:512]], axis=1)
    k_second = sample(4, next_corners, point)

    values = jnp.concatenate(last_low + [k_first, k_second, jnp.zeros((10, 512), f32)], axis=0)
    high, rest = halves(values)
    split_late[0:16, :] = high
    split_late[16:32, :] = rest

    def late_copy(k, column):
        return pltpu.make_async_remote_copy(
            src_ref=late.at[16 * k + column], dst_ref=late_in.at[me], send_sem=late_sems.at[0],
            recv_sem=late_sems.at[1], device_id=(goal_of(k), column), device_id_type=MESH)

    def deliver_late(pair, carry):
        rows = (2 * pair, 2 * pair + 1)
        for k in rows:
            parts = newest(chosen[k])
            for h in range(2):
                late[pl.ds(16 * k + 8 * h, 8), 0, :] = parts[h]
        send_rows(rows, late_copy)
        return carry

    lax.fori_loop(0, SPLIT // 2, deliver_late, 0)

    def deliver_all(pair, carry):
        rows = (2 * pair, 2 * pair + 1)
        for k in rows:
            parts = newest(fill(k))
            for h in range(2):
                message[pl.ds(16 * k + 8 * h, 8), EARLY, :] = parts[h]
        send_rows(rows, bulk(EARLY + 1))
        return carry

    lax.fori_loop(SPLIT // 2, 4, deliver_all, 0)
    own_late = pltpu.make_async_copy(late.at[tx], late_in.at[me], own_sems.at[1])
    own_late.start()

    end_ref[...] = rest_of_step(1, [all_corners(s) for s in (5, 6, 7)], point, k_second)

    def landed(number, rows):
        return arrived.at[pl.ds(0, number), pl.ds(0, rows)]

    def keep_late(sender, h, part):
        part = swap_blocks(part)
        for kind in range(3):
            late_ref[kind, sender, 2 * h : 2 * h + 2, :] = part[2 * kind : 2 * kind + 2]

    def place_row(k, carry):
        sender = lax.rem(ty - offset(k) + 8, 8)

        @pl.when(k == 0)
        def _():
            pltpu.make_async_copy(landed(15, EARLY), landed(15, EARLY), recv_sem.at[0]).wait()
            own_copy.wait()

        @pl.when((k > 0) & (k < SPLIT))
        def _():
            pltpu.make_async_copy(landed(16, EARLY), landed(16, EARLY), recv_sem.at[k]).wait()

        @pl.when(k >= SPLIT)
        def _():
            pltpu.make_async_copy(landed(16, EARLY + 1), landed(16, EARLY + 1), recv_sem.at[k]).wait()
            for h in range(2):
                keep_late(sender, h, arrived[pl.ds(sender * 16 + 8 * h, 8), EARLY, :])

        slab = slabs_ref.at[sender]
        for h in range(2):
            tiles = pl.ds(sender * 16 + 8 * h, 8)
            wide = jnp.transpose(arrived[tiles, 0:16, :].reshape(128, 128))
            for c in range(2):
                slab[pl.ds(2 * h + c, 64, stride=4), :] = wide[64 * c : 64 * c + 64]
                slab[pl.ds(64 * 4 + 2 * h + c, 8, stride=4), :] = swap_blocks(arrived[tiles, 16 + c, :])
        return carry

    lax.fori_loop(0, 8, place_row, 0)

    own_late.wait()
    few = 16 * SPLIT - 1
    sent = late.at[pl.ds(0, few)]
    pltpu.make_async_copy(sent, sent, late_sems.at[1]).wait()
    for k in range(SPLIT):
        sender = lax.rem(ty - offset(k) + 8, 8)
        for h in range(2):
            keep_late(sender, h, late_in[pl.ds(sender * 16 + 8 * h, 8), 0, :])
    for copy in edge_copies + packed_copies + spot_copies:
        copy.wait_send()
    pltpu.make_async_copy(sent, sent, late_sems.at[0]).wait()
    pltpu.make_async_copy(landed(few, EARLY), landed(few, EARLY), send_sems.at[0]).wait()
    rest = 128 - 16 * SPLIT
    pltpu.make_async_copy(landed(rest, EARLY + 1), landed(rest, EARLY + 1), send_sems.at[1]).wait()


def finish_kernel(slabs_ref, late_ref, filter_ref, out_ref, buffer, sems):
    matrix = filter_ref[...]
    weights = [jnp.broadcast_to(matrix[:, at : at + 1], (SAMPLES, 128)) for at in (HISTORY, HISTORY + 1)]
    copies = []
    for part in range(4):
        rows = buffer.at[part].reshape(SAMPLES * 8, 128)
        for r in range(8):
            at = 8 * part + r
            early = slabs_ref[at // 4, pl.ds(at % 4, SAMPLES - 1, stride=4), :]
            low = jnp.concatenate([early, late_ref[0, at // 4, at % 4 : at % 4 + 1, :]], axis=0)
            first, second = (late_ref[kind, at // 4, at % 4 : at % 4 + 1, :] for kind in (1, 2))
            rows[pl.ds(r, SAMPLES, stride=8), :] = low + weights[0] * first + weights[1] * second
        copies.append(pltpu.make_async_copy(buffer.at[part], out_ref.at[:, pl.ds(8 * part, 8), :], sems.at[part]))
        copies[-1].start()
    for copy in copies:
        copy.wait()


def per_device(velocity, start_position, cells, history, leavers, owner, filter_matrix):
    vmem = pl.BlockSpec(memory_space=pltpu.VMEM)
    hbm = pl.BlockSpec(memory_space=pl.ANY)
    slabs, late, end = pl.pallas_call(
        advance_kernel,
        out_shape=(
            pltpu.VMEM((8, 288, 128), f32),
            pltpu.VMEM((3, 8, 4, 128), f32),
            jax.ShapeDtypeStruct((2, 512), f32),
        ),
        in_specs=[pl.BlockSpec(memory_space=pltpu.SMEM), hbm, vmem, vmem, hbm, vmem, vmem],
        out_specs=(vmem, vmem, vmem),
        scratch_shapes=[
            pltpu.VMEM((2, 3, 128, 128), f32),
            pltpu.VMEM((HISTORY * 8, 128), f32),
            pltpu.VMEM((5, 256, 256), bf16),
            pltpu.VMEM((4, 8, 128), f32),
            pltpu.VMEM((8, 8, 128), f32),
            pltpu.VMEM((8, 16, 256), f32),
            pltpu.VMEM((8, 16, 256), f32),
            pltpu.VMEM((8, 128), f32),
            pltpu.VMEM((8, 8, 128), f32),
            pltpu.VMEM((8, 8, 512), f32),
            pltpu.VMEM((SPLIT, 512, 256), bf16),
            pltpu.VMEM((512, 128), i32),
            pltpu.VMEM((512, 256), bf16),
            pltpu.VMEM((32, 512), bf16),
            pltpu.VMEM((32, 512), bf16),
            pltpu.VMEM((128, 24, 128), f32),
            pltpu.VMEM((128, 24, 128), f32),
            pltpu.VMEM((16 * SPLIT, 1, 128), f32),
            pltpu.VMEM((128, 1, 128), f32),
        ]
        + [pltpu.SemaphoreType.DMA((8,))] * 6
        + [
            pltpu.SemaphoreType.DMA((2,)),
            pltpu.SemaphoreType.DMA((8,)),
            pltpu.SemaphoreType.DMA((2,)),
            pltpu.SemaphoreType.DMA((2,)),
            pltpu.SemaphoreType.DMA((2,)),
            pltpu.SemaphoreType.REGULAR,
        ],
        compiler_params=pltpu.CompilerParams(collective_id=0, has_side_effects=True),
        name="advance",
    )(
        leavers, velocity, start_position, cells.reshape(8, 2, 512),
        history.reshape(2, HISTORY, 4, 128).transpose(1, 2, 0, 3).reshape(HISTORY * 8, 128),
        owner.reshape(1, 512), filter_matrix,
    )
    out = pl.pallas_call(
        finish_kernel,
        out_shape=jax.ShapeDtypeStruct((SAMPLES, 32, 128), f32),
        in_specs=[vmem, vmem, vmem],
        out_specs=hbm,
        scratch_shapes=[pltpu.VMEM((4, SAMPLES, 8, 128), f32), pltpu.SemaphoreType.DMA((4,))],
        name="finish",
    )(
        pltpu.with_memory_space_constraint(slabs, pltpu.VMEM),
        pltpu.with_memory_space_constraint(late, pltpu.VMEM),
        filter_matrix,
    )
    return out.reshape(SAMPLES, 16, 2, 128).transpose(2, 0, 1, 3).reshape(2, SAMPLES, 2048)


def solution(mesh):
    placed = (
        P(None, None, "ty", "tx"),
        P(None, ("ty", "tx")),
        P(None, None, None, ("ty", "tx")),
        P(None, None, ("ty", "tx")),
        P(),
        P(("ty", "tx"), None),
        P(),
    )
    return jax.shard_map(
        per_device,
        mesh=mesh,
        in_specs=placed,
        out_specs=P(None, None, ("ty", "tx")),
        check_vma=False,
    )
```
